512 devices in a mesh: hyd: 8 (over y), tm: 16 (over z_hi, x), freq: 4 (over z_lo, core).
Axes of the slice: x: 4, y: 8, z: 8 (z_hi: 4, z_lo: 2; z = z_hi * 2 + z_lo), core: 2. Of those that a mesh axis runs over, the one named last changes fastest.
Arguments:
- spectra: bfloat16 [2, 16, 1024, 2048], P(None, 'tm', 'freq', 'hyd'), may hold values from -6 to 6
- row_lags: int32 [32, 512], replicated, may hold values from 0 to 31
- col_lags: int32 [64, 512], replicated, may hold values from 0 to 31
- replica: bfloat16 [2, 8192], replicated, may hold values from -0.0625 to 0.0625
- rep_len: int32 [1], replicated, may hold values from 4096 to 8192
Outputs:
- echoes: float32 [512, 2, 16384], P(('hyd', 'freq'), None, 'tm')
The draws below stay inside these ranges and needn't reach their ends.
All inputs are finite; a program needn't handle non-finite values.
Results may differ from the reference program's by a relative error of at most 0.011.
Values may be sent and summed in bfloat16 or wider, within the bound.
A program may use at most 64 MiB of HBM per device.

```python
import math
import jax
import jax.numpy as jnp
from jax import lax

ARRAY_ROWS = 32
ARRAY_COLS = 64
SENSORS = 2048
BEAMS = 512
BINS = 1024
FRAMES = 16
REPLICA = 8192


def touch_ends(entries, stream_key, low, high):
    extent = entries.shape
    place = [jax.random.randint(jax.random.fold_in(stream_key, axis), (), 0, extent[axis]) for axis in range(len(extent))]
    entries = entries.at[tuple(place)].set(low)
    longest = extent.index(max(extent))
    place[longest] = (place[longest] + 1) % extent[longest]
    return entries.at[tuple(place)].set(high)


def steps_of(stream_key, dims, pieces, smallest, top_value):
    gain = 1.0
    for position, parts in pieces:
        steps = jax.random.uniform(jax.random.fold_in(jax.random.fold_in(stream_key, 6), position), (parts,), jnp.float32, smallest / len(pieces), top_value / len(pieces))
        gain = gain * jnp.repeat(jnp.exp(steps), dims[position] // parts).reshape((-1,) + (1,) * (len(dims) - 1 - position))
    return gain


def gaussian(rng, shape, deviation, bound, split=(), kind=jnp.bfloat16):
    factor_of = steps_of(rng, shape, split, -0.22, 0.18) if split else 1.0
    entries = jax.random.normal(rng, shape, jnp.float32) * deviation * factor_of
    return jnp.minimum(jnp.maximum(entries, -bound), bound).astype(kind)


def setup_inputs(seed: int = 0) -> dict:
    splits = jax.random.split(jax.random.key(seed), 6)
    return {
        "spectra": gaussian(splits[0], (2, FRAMES, BINS, SENSORS), 1.0, 6.0, ((1, 16), (2, 4), (3, 8))),
        "row_lags": touch_ends(jax.random.randint(splits[1], (ARRAY_ROWS, BEAMS), 0, 32), jax.random.fold_in(splits[1], 1), 0, 31).astype(jnp.int32),
        "col_lags": touch_ends(jax.random.randint(splits[2], (ARRAY_COLS, BEAMS), 0, 32), jax.random.fold_in(splits[2], 1), 0, 31).astype(jnp.int32),
        "replica": gaussian(splits[3], (2, REPLICA), REPLICA ** -0.5, 0.0625),
        "rep_len": jax.random.randint(splits[4], (1,), REPLICA // 2, REPLICA + 1).astype(jnp.int32),
    }


two_pi = 2.0 * math.pi


def steering(bin_index, lag_table, factor):
    period = 2 * BINS
    phase = (bin_index[:, None, None] * lag_table[None]) % period
    angles = phase.astype(jnp.float32) * (two_pi / period)
    return (jnp.cos(angles) * factor).astype(jnp.bfloat16), (jnp.sin(angles) * factor).astype(jnp.bfloat16)


def highest(form, left, right):
    return jnp.einsum(form, left, right, precision=lax.Precision.HIGHEST)


def reference(spectra, row_lags, col_lags, replica, rep_len):
    frame_count = spectra.shape[1]
    bin_width = 16
    bin_blocks = BINS // bin_width
    arranged = spectra.reshape(2, frame_count, bin_blocks, bin_width, ARRAY_ROWS, ARRAY_COLS)
    arranged = jnp.transpose(arranged, (2, 3, 0, 1, 4, 5))
    chosen_bins = (BINS // 2 + jnp.arange(BINS, dtype=jnp.int32)).reshape(bin_blocks, bin_width)

    def one_block(pair_in):
        slab_in, block_bins = pair_in
        col_re, col_im = steering(block_bins, col_lags, ARRAY_COLS ** -0.5)
        col_re = col_re.astype(jnp.float32)
        col_im = col_im.astype(jnp.float32)
        data_re = slab_in[:, 0].astype(jnp.float32)
        data_im = slab_in[:, 1].astype(jnp.float32)
        along_re = highest("wtrc,wcb->wtrb", data_re, col_re) - highest("wtrc,wcb->wtrb", data_im, col_im)
        along_im = highest("wtrc,wcb->wtrb", data_re, col_im) + highest("wtrc,wcb->wtrb", data_im, col_re)
        row_re, row_im = steering(block_bins, row_lags, ARRAY_ROWS ** -0.5)
        row_re = row_re.astype(jnp.float32)[:, None]
        row_im = row_im.astype(jnp.float32)[:, None]
        beam_re = jnp.sum(along_re * row_re - along_im * row_im, axis=2)
        beam_im = jnp.sum(along_re * row_im + along_im * row_re, axis=2)
        return jnp.stack([beam_re, beam_im], axis=1).astype(jnp.bfloat16)

    beam_spectra = lax.map(one_block, (arranged, chosen_bins)).reshape(BINS, 2, frame_count, BEAMS)
    beam_spectra = lax.optimization_barrier(beam_spectra).astype(jnp.float32)
    samples = jnp.arange(BINS, dtype=jnp.int32)
    phase = (samples[:, None] * samples[None]) % BINS
    angles = phase.astype(jnp.float32) * (two_pi / BINS)
    tab_re = (jnp.cos(angles) * BINS ** -0.5).astype(jnp.bfloat16).astype(jnp.float32)
    tab_im = (jnp.sin(angles) * BINS ** -0.5).astype(jnp.bfloat16).astype(jnp.float32)
    spec_re = beam_spectra[:, 0]
    spec_im = beam_spectra[:, 1]
    series_re = highest("ftb,fn->tbn", spec_re, tab_re) - highest("ftb,fn->tbn", spec_im, tab_im)
    series_im = highest("ftb,fn->tbn", spec_re, tab_im) + highest("ftb,fn->tbn", spec_im, tab_re)
    series_re = lax.optimization_barrier(series_re.astype(jnp.bfloat16)).astype(jnp.float32)
    series_im = lax.optimization_barrier(series_im.astype(jnp.bfloat16)).astype(jnp.float32)
    time_total = frame_count * BINS
    series_re = jnp.transpose(series_re, (1, 0, 2)).reshape(BEAMS, time_total)
    series_im = jnp.transpose(series_im, (1, 0, 2)).reshape(BEAMS, time_total)
    kept_mask = jnp.arange(REPLICA, dtype=jnp.int32) < rep_len[0]
    pulse_re = jnp.where(kept_mask, replica[0].astype(jnp.float32), jnp.zeros((REPLICA,), jnp.float32))
    pulse_im = jnp.where(kept_mask, replica[1].astype(jnp.float32), jnp.zeros((REPLICA,), jnp.float32))
    length = time_total + REPLICA
    signal = series_re + 1j * series_im
    pulse = pulse_re + 1j * pulse_im
    signal_f = jnp.fft.fft(signal, n=length, axis=1)
    pulse_f = jnp.fft.fft(pulse, n=length)
    corr = jnp.fft.ifft(signal_f * jnp.conj(pulse_f)[None], axis=1)[:, :time_total]
    return jnp.stack([jnp.real(corr), jnp.imag(corr)], axis=1).astype(jnp.float32)
```

```python
import math

import jax
import jax.numpy as jnp
import numpy as np
from jax import lax
from jax.experimental import pallas as pl
from jax.experimental.pallas import tpu as pltpu
from jax.sharding import PartitionSpec as P

ROWS = 32
COLS = 64
BINS = 1024
BEAMS = 512
FRAMES = 16
REPLICA = 8192
PERIOD = 2 * BINS
LOCAL_BINS = 32
TAPS = REPLICA // 128 + 1


def start_powers():
    table = np.zeros((32, 16), np.float64)
    for place in range(32):
        first = BINS // 2 + place * LOCAL_BINS
        for bit in range(5):
            angle = 2.0 * math.pi * ((first << bit) % PERIOD) / PERIOD
            table[place, 2 * bit] = math.cos(angle)
            table[place, 2 * bit + 1] = math.sin(angle)
    return table.reshape(-1).astype(np.float32)


def inverse_factors():
    n = np.arange(BINS)
    fine = np.exp(2j * np.pi * ((np.arange(32)[:, None] * n) % BINS) / BINS) / math.sqrt(BINS)
    source = np.arange(32)
    first = (source % 4) * 256 + (source // 4) * 32
    coarse = np.exp(2j * np.pi * ((first[:, None] * n) % BINS) / BINS)
    return tuple(part.astype(np.float32) for part in (fine.real, fine.imag, coarse.real, coarse.imag))


def steer(lags, powers, factor):
    re, im = None, None
    for bit in range(5):
        pr, pi = powers[bit]
        chosen = (lags & (1 << bit)) != 0
        if re is None:
            re = jnp.where(chosen, pr * factor, jnp.full(lags.shape, factor, jnp.float32))
            im = jnp.where(chosen, pi * factor, jnp.zeros(lags.shape, jnp.float32))
        else:
            moved_re = re * pr - im * pi
            moved_im = re * pi + im * pr
            re = jnp.where(chosen, moved_re, re)
            im = jnp.where(chosen, moved_im, im)
    return re, im


def begin_steering(place, powers_ref, col_lags_ref, row_lags_ref, col, col_step, row, row_step):
    first = [
        (powers_ref[place * 16 + 2 * bit], powers_ref[place * 16 + 2 * bit + 1]) for bit in range(5)
    ]
    step = [
        (
            np.float32(math.cos(2.0 * math.pi * (1 << bit) / PERIOD)),
            np.float32(math.sin(2.0 * math.pi * (1 << bit) / PERIOD)),
        )
        for bit in range(5)
    ]
    for lags_ref, state, change, count, factor in (
        (col_lags_ref, col, col_step, COLS, COLS**-0.5),
        (row_lags_ref, row, row_step, ROWS, ROWS**-0.5),
    ):

        @pl.loop(0, count // 8)
        def _(group):
            rows = pl.ds(pl.multiple_of(group * 8, 8), 8)
            lags = lags_ref[rows, :]
            re, im = steer(lags, first, np.float32(factor))
            state[rows, 0:BEAMS] = re
            state[rows, BEAMS : 2 * BEAMS] = im
            re, im = steer(lags, step, np.float32(1.0))
            change[rows, 0:BEAMS] = re
            change[rows, BEAMS : 2 * BEAMS] = im


def advance(state, change, rows):
    re = state[rows, 0:BEAMS]
    im = state[rows, BEAMS : 2 * BEAMS]
    cr = change[rows, 0:BEAMS]
    ci = change[rows, BEAMS : 2 * BEAMS]
    state[rows, 0:BEAMS] = re * cr - im * ci
    state[rows, BEAMS : 2 * BEAMS] = re * ci + im * cr
    return re, im


def arrange_sensors(get, sensors):
    low = lax.broadcasted_iota(jnp.int32, (LOCAL_BINS, 128), 1) < 64
    for source in range(8):
        for pair in range(2):
            re = get(0, source, pair).astype(jnp.float32)
            im = get(1, source, pair).astype(jnp.float32)
            row = source * 4 + pair * 2
            sensors[row * 32 : row * 32 + 32, :] = jnp.where(low, re, pltpu.roll(im, 64, 1))
            row = row + 1
            sensors[row * 32 : row * 32 + 32, :] = jnp.where(low, pltpu.roll(re, 64, 1), im)


def beamform_kernel(
    powers_ref, spectra_ref, col_lags_ref, row_lags_ref, out_ref, col, col_step, row, row_step, weights, sensors
):
    place = lax.axis_index("freq") * 8 + lax.axis_index("hyd")
    begin_steering(place, powers_ref, col_lags_ref, row_lags_ref, col, col_step, row, row_step)
    arrange_sensors(
        lambda part, source, pair: spectra_ref[part, source, :, 128 * pair : 128 * pair + 128], sensors
    )

    @pl.loop(0, LOCAL_BINS)
    def _(bin_at):
        for group in range(COLS // 16):
            rows = slice(16 * group, 16 * group + 16)
            re, im = advance(col, col_step, rows)
            weights[rows, 0:BEAMS] = re.astype(jnp.bfloat16)
            weights[rows, BEAMS : 2 * BEAMS] = im.astype(jnp.bfloat16)
            rows = slice(64 + 16 * group, 64 + 16 * group + 16)
            weights[rows, 0:BEAMS] = (-im).astype(jnp.bfloat16)
            weights[rows, BEAMS : 2 * BEAMS] = re.astype(jnp.bfloat16)
        data = sensors[pl.ds(bin_at, 32, stride=32), :].astype(jnp.bfloat16)
        along = jnp.dot(data, weights[...], preferred_element_type=jnp.float32)
        row_re, row_im = advance(row, row_step, slice(0, 32))
        along_re = along[:, 0:BEAMS]
        along_im = along[:, BEAMS:]
        out_ref[pl.ds(bin_at, 1), :] = jnp.sum(along_re * row_re - along_im * row_im, axis=0, keepdims=True)
        out_ref[pl.ds(32 + bin_at, 1), :] = jnp.sum(along_re * row_im + along_im * row_re, axis=0, keepdims=True)


def build_toeplitz(reversed_ref, toeplitz):
    down = lax.broadcasted_iota(jnp.int32, (128, 128), 0)
    across = lax.broadcasted_iota(jnp.int32, (128, 128), 1)
    upper = across >= down

    def circulant(part, tap):
        line = jnp.broadcast_to(reversed_ref[part, pl.ds(tap, 1), :], (128, 128))
        return pltpu.roll(line, 0, 1, stride=1, stride_axis=0)

    @pl.loop(0, TAPS)
    def _(tap):
        rows = pl.ds(pl.multiple_of(tap * 128, 128), 128)
        for part in range(2):
            here = circulant(part, tap)
            after = circulant(part, tap + 1)
            toeplitz[rows, 128 * part : 128 * part + 128] = jnp.where(upper, here, after).astype(jnp.bfloat16)


def build_inverse(fine_re_ref, fine_im_ref, coarse_re_ref, coarse_im_ref, table):
    @pl.loop(0, 32)
    def _(source):
        start = pl.multiple_of(source * 64, 64)
        for half in range(2):
            for block in range(4):
                cols = slice(256 * block, 256 * block + 256)
                fr = fine_re_ref[16 * half : 16 * half + 16, cols]
                fi = fine_im_ref[16 * half : 16 * half + 16, cols]
                cr = coarse_re_ref[pl.ds(source, 1), cols]
                ci = coarse_im_ref[pl.ds(source, 1), cols]
                re = fr * cr - fi * ci
                im = fr * ci + fi * cr
                rows = pl.ds(start + 16 * half, 16)
                table[rows, cols] = re.astype(jnp.bfloat16)
                table[rows, slice(1024 + 256 * block, 1280 + 256 * block)] = im.astype(jnp.bfloat16)
                rows = pl.ds(start + 32 + 16 * half, 16)
                table[rows, cols] = (-im).astype(jnp.bfloat16)
                table[rows, slice(1024 + 256 * block, 1280 + 256 * block)] = re.astype(jnp.bfloat16)


def invert(gathered, table, series):
    series[...] = jnp.zeros_like(series)
    for block in range(8):
        cols = slice(256 * block, 256 * block + 256)
        part, first = block // 4, 2 * (block % 4)
        total = jnp.dot(gathered, table[:, cols], preferred_element_type=jnp.float32)
        for side in range(2):
            series[part, first + side, 0:16, :] = total[:, 128 * side : 128 * side + 128]


def spread(series, blocks):
    for part in range(2):
        for index in range(72):
            ahead, block = index // 8, index % 8
            blocks[part, 16 * index : 16 * index + 16, :] = series[part, block, ahead : ahead + 16, :].astype(
                jnp.bfloat16
            )


def correlate(blocks, toeplitz, total):
    def lines(tap):
        return jnp.concatenate(
            [blocks[part, pl.ds(pl.multiple_of(tap * 16, 16), 128), :] for part in range(2)], axis=0
        )

    last = TAPS - 1
    total[...] = jnp.dot(lines(last), toeplitz[128 * last : 128 * TAPS, :], preferred_element_type=jnp.float32)

    @pl.loop(0, last // 8)
    def _(group):
        tap = group * 8
        data = jnp.concatenate([lines(tap + member) for member in range(8)], axis=1)
        weights = toeplitz[pl.ds(pl.multiple_of(tap * 128, 1024), 1024), :]
        total[...] += jnp.dot(data, weights, preferred_element_type=jnp.float32)


def filter_kernel(
    gathered_ref,
    reversed_ref,
    fine_re_ref,
    fine_im_ref,
    coarse_re_ref,
    coarse_im_ref,
    out_ref,
    toeplitz,
    table,
    series,
    blocks,
    total,
):
    build_toeplitz(reversed_ref, toeplitz)
    build_inverse(fine_re_ref, fine_im_ref, coarse_re_ref, coarse_im_ref, table)
    invert(gathered_ref[...], table, series)
    spread(series, blocks)
    correlate(blocks, toeplitz, total)
    out_ref[0] = total[0:128, 0:128] + total[128:256, 128:256]
    out_ref[1] = total[128:256, 0:128] - total[0:128, 128:256]


def in_vmem(count):
    return [pl.BlockSpec(memory_space=pltpu.VMEM)] * count


def beamform(spectra, col_lags, row_lags):
    return pl.pallas_call(
        beamform_kernel,
        out_shape=jax.ShapeDtypeStruct((64, BEAMS), jnp.float32),
        in_specs=[pl.BlockSpec(memory_space=pltpu.SMEM)] + in_vmem(3),
        out_specs=in_vmem(1)[0],
        scratch_shapes=[
            pltpu.VMEM((COLS, 2 * BEAMS), jnp.float32),
            pltpu.VMEM((COLS, 2 * BEAMS), jnp.float32),
            pltpu.VMEM((ROWS, 2 * BEAMS), jnp.float32),
            pltpu.VMEM((ROWS, 2 * BEAMS), jnp.float32),
            pltpu.VMEM((128, 2 * BEAMS), jnp.bfloat16),
            pltpu.VMEM((1024, 128), jnp.float32),
        ],
    )(jnp.asarray(start_powers()), spectra, col_lags, row_lags)


def matched(gathered, reversed_pulse):
    factors = [jnp.asarray(part) for part in inverse_factors()]
    return pl.pallas_call(
        filter_kernel,
        out_shape=jax.ShapeDtypeStruct((2, 128, 128), jnp.float32),
        in_specs=in_vmem(6),
        out_specs=in_vmem(1)[0],
        scratch_shapes=[
            pltpu.VMEM((TAPS * 128, 256), jnp.bfloat16),
            pltpu.VMEM((2048, 2048), jnp.bfloat16),
            pltpu.VMEM((2, 8, 24, 128), jnp.float32),
            pltpu.VMEM((2, 72 * 16, 128), jnp.bfloat16),
            pltpu.VMEM((256, 256), jnp.float32),
        ],
    )(gathered, reversed_pulse, *factors)


def reverse_pulse(replica, rep_len):
    kept = jnp.arange(REPLICA, dtype=jnp.int32) < rep_len[0]
    masked = jnp.where(kept[None], replica, jnp.zeros_like(replica)).astype(jnp.float32)
    padded = jnp.pad(masked, ((0, 0), (127, (TAPS + 1) * 128 - 127 - REPLICA)))
    return jnp.flip(padded.reshape(2, TAPS + 1, 128), axis=2)


def on_device(spectra, row_lags, col_lags, replica, rep_len):
    moved = lax.all_to_all(
        spectra.reshape(2, 8, LOCAL_BINS, 256), "hyd", split_axis=1, concat_axis=1, tiled=True
    )
    reversed_pulse = reverse_pulse(replica, rep_len)
    formed = beamform(moved, col_lags, row_lags)
    formed = formed.astype(jnp.bfloat16).T
    arrived = lax.all_to_all(formed, ("hyd", "freq"), split_axis=0, concat_axis=0, tiled=True)
    arranged = jnp.transpose(arrived.reshape(32, 16, 64), (1, 0, 2)).reshape(16, 2048)
    gathered = lax.all_to_all(arranged, "tm", split_axis=0, concat_axis=0, tiled=True)
    echoes = matched(gathered, reversed_pulse)
    echoes = jnp.transpose(echoes.reshape(2, 8, 16, 128), (2, 0, 1, 3)).reshape(16, 2 * BINS)
    returned = lax.all_to_all(echoes, "tm", split_axis=0, concat_axis=0, tiled=True)
    return returned.reshape(16, 2, BINS)


def solution(mesh):
    placed = (P(None, "tm", "freq", "hyd"), P(), P(), P(), P())
    return jax.shard_map(
        on_device,
        mesh=mesh,
        in_specs=placed,
        out_specs=P(("hyd", "freq"), None, "tm"),
        check_vma=False,
    )
```

```python
import math

import jax
import jax.numpy as jnp
import numpy as np
from jax import lax
from jax.experimental import pallas as pl
from jax.experimental.pallas import tpu as pltpu
from jax.sharding import PartitionSpec as P

ROWS = 32
COLS = 64
BINS = 1024
BEAMS = 512
FRAMES = 16
REPLICA = 8192
PERIOD = 2 * BINS
LOCAL_BINS = 32
TAPS = REPLICA // 128 + 1


def start_powers():
    table = np.zeros((32, 16), np.float64)
    for place in range(32):
        first = BINS // 2 + place * LOCAL_BINS
        for bit in range(5):
            angle = 2.0 * math.pi * ((first << bit) % PERIOD) / PERIOD
            table[place, 2 * bit] = math.cos(angle)
            table[place, 2 * bit + 1] = math.sin(angle)
    return table.reshape(-1).astype(np.float32)


def inverse_factors():
    n = np.arange(BINS)
    fine = np.exp(2j * np.pi * ((np.arange(32)[:, None] * n) % BINS) / BINS) / math.sqrt(BINS)
    source = np.arange(32)
    first = (source % 4) * 256 + (source // 4) * 32
    coarse = np.exp(2j * np.pi * ((first[:, None] * n) % BINS) / BINS)
    return tuple(part.astype(np.float32) for part in (fine.real, fine.imag, coarse.real, coarse.imag))


def steer(lags, powers, factor):
    re, im = None, None
    for bit in range(5):
        pr, pi = powers[bit]
        chosen = (lags & (1 << bit)) != 0
        if re is None:
            re = jnp.where(chosen, pr * factor, jnp.full(lags.shape, factor, jnp.float32))
            im = jnp.where(chosen, pi * factor, jnp.zeros(lags.shape, jnp.float32))
        else:
            moved_re = re * pr - im * pi
            moved_im = re * pi + im * pr
            re = jnp.where(chosen, moved_re, re)
            im = jnp.where(chosen, moved_im, im)
    return re, im


def begin_steering(place, powers_ref, col_lags_ref, row_lags_ref, col, col_step, row, row_step):
    first = [
        (powers_ref[place * 16 + 2 * bit], powers_ref[place * 16 + 2 * bit + 1]) for bit in range(5)
    ]
    step = [
        (
            np.float32(math.cos(2.0 * math.pi * (1 << bit) / PERIOD)),
            np.float32(math.sin(2.0 * math.pi * (1 << bit) / PERIOD)),
        )
        for bit in range(5)
    ]
    for lags_ref, state, change, count, factor in (
        (col_lags_ref, col, col_step, COLS, COLS**-0.5),
        (row_lags_ref, row, row_step, ROWS, ROWS**-0.5),
    ):

        @pl.loop(0, count // 8)
        def _(group):
            rows = pl.ds(pl.multiple_of(group * 8, 8), 8)
            lags = lags_ref[rows, :]
            re, im = steer(lags, first, np.float32(factor))
            state[rows, 0:BEAMS] = re
            state[rows, BEAMS : 2 * BEAMS] = im
            re, im = steer(lags, step, np.float32(1.0))
            change[rows, 0:BEAMS] = re
            change[rows, BEAMS : 2 * BEAMS] = im


def advance(state, change, rows):
    re = state[rows, 0:BEAMS]
    im = state[rows, BEAMS : 2 * BEAMS]
    cr = change[rows, 0:BEAMS]
    ci = change[rows, BEAMS : 2 * BEAMS]
    state[rows, 0:BEAMS] = re * cr - im * ci
    state[rows, BEAMS : 2 * BEAMS] = re * ci + im * cr
    return re, im


def arrange_sensors(arrived, sensors):
    low = lax.broadcasted_iota(jnp.int32, (LOCAL_BINS, 128), 1) < 64
    for source in range(8):
        for pair in range(2):
            cols = slice(128 * pair, 128 * pair + 128)
            re = arrived[source, 0, :, cols].astype(jnp.float32)
            im = arrived[source, 1, :, cols].astype(jnp.float32)
            row = source * 4 + pair * 2
            sensors[row * 32 : row * 32 + 32, :] = jnp.where(low, re, pltpu.roll(im, 64, 1))
            row = row + 1
            sensors[row * 32 : row * 32 + 32, :] = jnp.where(low, pltpu.roll(re, 64, 1), im)


def build_steering(col, col_step, row, row_step, weights, row_table):
    @pl.loop(0, LOCAL_BINS)
    def _(bin_at):
        for group in range(COLS // 16):
            rows = slice(16 * group, 16 * group + 16)
            re, im = advance(col, col_step, rows)
            weights[bin_at, rows, 0:BEAMS] = re.astype(jnp.bfloat16)
            weights[bin_at, rows, BEAMS : 2 * BEAMS] = im.astype(jnp.bfloat16)
            rows = slice(64 + 16 * group, 64 + 16 * group + 16)
            weights[bin_at, rows, 0:BEAMS] = (-im).astype(jnp.bfloat16)
            weights[bin_at, rows, BEAMS : 2 * BEAMS] = re.astype(jnp.bfloat16)
        for group in range(ROWS // 8):
            rows = slice(8 * group, 8 * group + 8)
            re, im = advance(row, row_step, rows)
            row_table[bin_at, rows, 0:BEAMS] = re
            row_table[bin_at, rows, BEAMS : 2 * BEAMS] = im


def form_beams(sensors, weights, row_table, formed):
    formed[64:128, :] = jnp.zeros((64, BEAMS), jnp.float32)

    @pl.loop(0, LOCAL_BINS)
    def _(bin_at):
        data = sensors[pl.ds(bin_at, 32, stride=32), :].astype(jnp.bfloat16)
        along = jnp.dot(data, weights[bin_at], preferred_element_type=jnp.float32)
        row_re = row_table[bin_at, :, 0:BEAMS]
        row_im = row_table[bin_at, :, BEAMS : 2 * BEAMS]
        along_re = along[:, 0:BEAMS]
        along_im = along[:, BEAMS:]
        formed[pl.ds(bin_at, 1), :] = jnp.sum(along_re * row_re - along_im * row_im, axis=0, keepdims=True)
        formed[pl.ds(32 + bin_at, 1), :] = jnp.sum(along_re * row_im + along_im * row_re, axis=0, keepdims=True)


def pack_groups(formed, groups):
    low = lax.broadcasted_iota(jnp.int32, (8, 128), 1) < 64
    for quarter in range(4):
        turned = formed[:, 128 * quarter : 128 * quarter + 128].T
        for member in range(8):
            first = turned[16 * member : 16 * member + 8]
            second = turned[16 * member + 8 : 16 * member + 16]
            packed = jnp.where(low, first, pltpu.roll(second, 64, 1))
            groups[8 * quarter + member] = packed.astype(jnp.bfloat16)


def pack_beams(arrived, work, beams):
    low = lax.broadcasted_iota(jnp.int32, (8, 128), 1) < 64
    for pair in range(16):
        first = arrived[2 * pair].astype(jnp.float32)
        second = arrived[2 * pair + 1].astype(jnp.float32)
        work[8 * pair : 8 * pair + 8, :] = jnp.where(low, first, pltpu.roll(second, 64, 1))
        work[128 + 8 * pair : 136 + 8 * pair, :] = jnp.where(low, pltpu.roll(first, 64, 1), second)
    for beam in range(16):
        start = 128 * (beam // 8) + beam % 8
        beams[beam] = work[pl.ds(start, 16, stride=8), :].astype(jnp.bfloat16)


def gather_frames(arrived, work, gathered):
    for frame in range(FRAMES):
        work[16 * frame : 16 * frame + 16, :] = arrived[frame].astype(jnp.float32)
    for pair in range(16):
        gathered[:, 128 * pair : 128 * pair + 128] = work[pl.ds(pair, 16, stride=16), :].astype(jnp.bfloat16)


def lay_pulse(replica, length, lines, mirrored):
    lines[...] = jnp.zeros_like(lines)
    lane = lax.broadcasted_iota(jnp.int32, (2, 128), 1)
    for tap in range(TAPS - 1):
        line = replica[:, 128 * tap : 128 * tap + 128].astype(jnp.float32)
        lines[2 + 2 * tap : 4 + 2 * tap, :] = jnp.where(lane + 128 * tap < length, line, 0.0)
    down = lax.broadcasted_iota(jnp.int32, (128, 128), 0)
    across = lax.broadcasted_iota(jnp.int32, (128, 128), 1)
    turn = jnp.where((down + across) % 128 == 0, 1.0, 0.0).astype(jnp.bfloat16)
    mirrored[...] = jnp.dot(lines[...].astype(jnp.bfloat16), turn, preferred_element_type=jnp.float32)


def build_toeplitz(mirrored, toeplitz):
    down = lax.broadcasted_iota(jnp.int32, (128, 128), 0)
    across = lax.broadcasted_iota(jnp.int32, (128, 128), 1)
    lower = down >= across

    @pl.loop(0, TAPS)
    def _(tap):
        rows = pl.ds(pl.multiple_of(tap * 128, 128), 128)
        for part in range(2):
            both = []
            for later in range(2):
                line = mirrored[pl.ds(2 * tap + 2 * later + part, 1), :]
                both.append(pltpu.roll(jnp.broadcast_to(line, (128, 128)), 0, 1, stride=1, stride_axis=0))
            toeplitz[rows, 128 * part : 128 * part + 128] = jnp.where(lower, both[1], both[0]).astype(jnp.bfloat16)

def build_inverse(fine_re_ref, fine_im_ref, coarse_re_ref, coarse_im_ref, table):
    @pl.loop(0, 32)
    def _(source):
        start = pl.multiple_of(source * 64, 64)
        for half in range(2):
            for block in range(4):
                cols = slice(256 * block, 256 * block + 256)
                fr = fine_re_ref[16 * half : 16 * half + 16, cols]
                fi = fine_im_ref[16 * half : 16 * half + 16, cols]
                cr = coarse_re_ref[pl.ds(source, 1), cols]
                ci = coarse_im_ref[pl.ds(source, 1), cols]
                re = fr * cr - fi * ci
                im = fr * ci + fi * cr
                rows = pl.ds(start + 16 * half, 16)
                table[rows, cols] = re.astype(jnp.bfloat16)
                table[rows, slice(1024 + 256 * block, 1280 + 256 * block)] = im.astype(jnp.bfloat16)
                rows = pl.ds(start + 32 + 16 * half, 16)
                table[rows, cols] = (-im).astype(jnp.bfloat16)
                table[rows, slice(1024 + 256 * block, 1280 + 256 * block)] = re.astype(jnp.bfloat16)


def invert(gathered, table, series):
    series[...] = jnp.zeros_like(series)
    for block in range(8):
        cols = slice(256 * block, 256 * block + 256)
        part, first = block // 4, 2 * (block % 4)
        total = jnp.dot(gathered, table[:, cols], preferred_element_type=jnp.float32)
        for side in range(2):
            series[part, first + side, 0:16, :] = total[:, 128 * side : 128 * side + 128]


def spread(series, blocks):
    for part in range(2):
        for index in range(72):
            ahead, block = index // 8, index % 8
            blocks[part, 16 * index : 16 * index + 16, :] = series[part, block, ahead : ahead + 16, :].astype(
                jnp.bfloat16
            )


def correlate(blocks, toeplitz, total):
    def lines(tap):
        return jnp.concatenate(
            [blocks[part, pl.ds(pl.multiple_of(tap * 16, 16), 128), :] for part in range(2)], axis=0
        )

    last = TAPS - 1
    total[...] = jnp.dot(lines(last), toeplitz[128 * last : 128 * TAPS, :], preferred_element_type=jnp.float32)

    @pl.loop(0, last // 8)
    def _(group):
        tap = group * 8
        data = jnp.concatenate([lines(tap + member) for member in range(8)], axis=1)
        weights = toeplitz[pl.ds(pl.multiple_of(tap * 128, 1024), 1024), :]
        total[...] += jnp.dot(data, weights, preferred_element_type=jnp.float32)


def send(source, target, sends, receives, slot, mine, device):
    return pltpu.make_async_remote_copy(
        src_ref=source,
        dst_ref=target,
        send_sem=sends.at[slot],
        recv_sem=receives.at[mine],
        device_id=device,
        device_id_type=pl.DeviceIdType.MESH,
    )


def ping_kernel(
    powers_ref,
    length_ref,
    spectra_hbm,
    col_lags_hbm,
    row_lags_hbm,
    replica_hbm,
    factors_hbm,
    out_hbm,
    spectra,
    col_lags,
    row_lags,
    replica,
    factors,
    arrived_bins,
    col,
    col_step,
    row,
    row_step,
    weights,
    row_table,
    sensors,
    formed,
    groups,
    arrived_groups,
    work,
    beams,
    arrived_beams,
    gathered,
    lines,
    mirrored,
    toeplitz,
    table,
    series,
    blocks,
    total,
    leaving,
    returned,
    local_sem,
    bin_send,
    bin_recv,
    group_send,
    group_recv,
    beam_send,
    beam_recv,
    out_send,
    out_recv,
):
    hyd = lax.axis_index("hyd")
    freq = lax.axis_index("freq")
    tm = lax.axis_index("tm")
    owner = hyd * 4 + freq

    def owner_at(index):
        return {"hyd": index // 4, "freq": index % 4}

    barrier = pltpu.get_barrier_semaphore()

    @pl.loop(1, 32)
    def _(away):
        pl.semaphore_signal(
            barrier, inc=1, device_id=owner_at((owner + away) % 32), device_id_type=pl.DeviceIdType.MESH
        )

    @pl.loop(1, 16)
    def _(away):
        pl.semaphore_signal(
            barrier, inc=1, device_id={"tm": (tm + away) % 16}, device_id_type=pl.DeviceIdType.MESH
        )

    inputs = [
        pltpu.make_async_copy(source, target, local_sem.at[index])
        for index, (source, target) in enumerate(
            (
                (col_lags_hbm, col_lags),
                (row_lags_hbm, row_lags),
                (spectra_hbm.at[:, 0], spectra),
                (replica_hbm, replica),
                (factors_hbm, factors),
            )
        )
    ]
    for copy in inputs:
        copy.start()
    inputs[0].wait()
    inputs[1].wait()
    begin_steering(freq * 8 + hyd, powers_ref, col_lags, row_lags, col, col_step, row, row_step)
    inputs[2].wait()
    pl.semaphore_wait(barrier, 46)

    def bins_of(place):
        return spectra.at[:, pl.ds(pl.multiple_of(place * LOCAL_BINS, LOCAL_BINS), LOCAL_BINS), :]

    sent = []
    for away in (4, 3, 5, 2, 6, 1, 7):
        place = (hyd + away) % 8
        copy = send(bins_of(place), arrived_bins.at[hyd], bin_send, bin_recv, away, hyd, {"hyd": place})
        copy.start()
        sent.append(copy)
    own = pltpu.make_async_copy(bins_of(hyd), arrived_bins.at[hyd], local_sem.at[5])
    own.start()

    build_steering(col, col_step, row, row_step, weights, row_table)
    inputs[3].wait()
    inputs[4].wait()
    lay_pulse(replica, length_ref[0], lines, mirrored)
    build_toeplitz(mirrored, toeplitz)
    build_inverse(factors.at[0], factors.at[1], factors.at[2], factors.at[3], table)

    own.wait()
    for away in range(1, 8):
        place = (hyd + away) % 8
        send(bins_of(place), arrived_bins.at[place], bin_send, bin_recv, away, place, {"hyd": place}).wait_recv()
    arrange_sensors(arrived_bins, sensors)
    form_beams(sensors, weights, row_table, formed)
    pack_groups(formed, groups)

    def group_copy(away, source):
        place = (owner + away) % 32
        return send(groups.at[place], arrived_groups.at[source], group_send, group_recv, away, source, owner_at(place))

    @pl.loop(1, 32)
    def _(away):
        group_copy(away, owner).start()

    own = pltpu.make_async_copy(groups.at[owner], arrived_groups.at[owner], local_sem.at[5])
    own.start()
    own.wait()

    @pl.loop(1, 32)
    def _(away):
        group_copy(away, (owner + away) % 32).wait_recv()

    pack_beams(arrived_groups, work, beams)

    def beam_copy(away, source):
        place = (tm + away) % 16
        return send(beams.at[place], arrived_beams.at[source], beam_send, beam_recv, away, source, {"tm": place})

    @pl.loop(1, 16)
    def _(away):
        beam_copy(away, tm).start()

    own = pltpu.make_async_copy(beams.at[tm], arrived_beams.at[tm], local_sem.at[5])
    own.start()
    own.wait()

    @pl.loop(1, 16)
    def _(away):
        beam_copy(away, (tm + away) % 16).wait_recv()

    gather_frames(arrived_beams, work, gathered)
    invert(gathered[...], table, series)
    spread(series, blocks)
    correlate(blocks, toeplitz, total)
    for block in range(8):
        rows = slice(16 * block, 16 * block + 16)
        after = slice(128 + 16 * block, 144 + 16 * block)
        work[pl.ds(block, 16, stride=16), :] = total[rows, 0:128] + total[after, 128:256]
        work[pl.ds(8 + block, 16, stride=16), :] = total[after, 0:128] - total[rows, 128:256]
    for frame in range(FRAMES):
        leaving[frame] = work[16 * frame : 16 * frame + 16, :].astype(jnp.bfloat16)

    def out_copy(away, source):
        place = (tm + away) % 16
        return send(leaving.at[place], returned.at[source], out_send, out_recv, away, source, {"tm": place})

    @pl.loop(1, 16)
    def _(away):
        out_copy(away, tm).start()

    own = pltpu.make_async_copy(leaving.at[tm], returned.at[tm], local_sem.at[5])
    own.start()
    own.wait()

    @pl.loop(1, 16)
    def _(away):
        out_copy(away, (tm + away) % 16).wait_recv()

    done = pltpu.make_async_copy(returned, out_hbm, local_sem.at[5])
    done.start()
    for copy in sent:
        copy.wait_send()

    @pl.loop(1, 32)
    def _(away):
        group_copy(away, owner).wait_send()

    @pl.loop(1, 16)
    def _(away):
        beam_copy(away, tm).wait_send()
        out_copy(away, tm).wait_send()

    done.wait()


def ping(spectra, row_lags, col_lags, replica, rep_len):
    factors = jnp.asarray(np.stack(inverse_factors()))
    smem = pl.BlockSpec(memory_space=pltpu.SMEM)
    hbm = pl.BlockSpec(memory_space=pl.ANY)
    bf16, f32, i32 = jnp.bfloat16, jnp.float32, jnp.int32
    dma = pltpu.SemaphoreType.DMA
    return pl.pallas_call(
        ping_kernel,
        out_shape=jax.ShapeDtypeStruct((16, 16, 128), bf16),
        in_specs=[smem, smem] + [hbm] * 5,
        out_specs=hbm,
        scratch_shapes=[
            pltpu.VMEM((2, 256, 256), bf16),
            pltpu.VMEM((COLS, BEAMS), i32),
            pltpu.VMEM((ROWS, BEAMS), i32),
            pltpu.VMEM((2, REPLICA), bf16),
            pltpu.VMEM((4, 32, BINS), f32),
            pltpu.VMEM((8, 2, LOCAL_BINS, 256), bf16),
            pltpu.VMEM((COLS, 2 * BEAMS), f32),
            pltpu.VMEM((COLS, 2 * BEAMS), f32),
            pltpu.VMEM((ROWS, 2 * BEAMS), f32),
            pltpu.VMEM((ROWS, 2 * BEAMS), f32),
            pltpu.VMEM((LOCAL_BINS, 128, 2 * BEAMS), bf16),
            pltpu.VMEM((LOCAL_BINS, ROWS, 2 * BEAMS), f32),
            pltpu.VMEM((1024, 128), f32),
            pltpu.VMEM((128, BEAMS), f32),
            pltpu.VMEM((32, 8, 128), bf16),
            pltpu.VMEM((32, 8, 128), bf16),
            pltpu.VMEM((256, 128), f32),
            pltpu.VMEM((16, 16, 128), bf16),
            pltpu.VMEM((16, 16, 128), bf16),
            pltpu.VMEM((16, 2048), bf16),
            pltpu.VMEM((144, 128), f32),
            pltpu.VMEM((144, 128), f32),
            pltpu.VMEM((TAPS * 128, 256), bf16),
            pltpu.VMEM((2048, 2048), bf16),
            pltpu.VMEM((2, 8, 24, 128), f32),
            pltpu.VMEM((2, 72 * 16, 128), bf16),
            pltpu.VMEM((256, 256), f32),
            pltpu.VMEM((16, 16, 128), bf16),
            pltpu.VMEM((16, 16, 128), bf16),
            dma((6,)),
            dma((8,)),
            dma((8,)),
            dma((32,)),
            dma((32,)),
            dma((16,)),
            dma((16,)),
            dma((16,)),
            dma((16,)),
        ],
        compiler_params=pltpu.CompilerParams(
            collective_id=0, has_side_effects=True, vmem_limit_bytes=60 * 1024 * 1024
        ),
    )(jnp.asarray(start_powers()), rep_len, spectra, col_lags, row_lags, replica, factors)


def on_device(spectra, row_lags, col_lags, replica, rep_len):
    returned = ping(spectra, row_lags, col_lags, replica, rep_len)
    return returned.astype(jnp.float32).reshape(16, 2, BINS)


def solution(mesh):
    placed = (P(None, "tm", "freq", "hyd"), P(), P(), P(), P())
    return jax.shard_map(
        on_device,
        mesh=mesh,
        in_specs=placed,
        out_specs=P(("hyd", "freq"), None, "tm"),
        check_vma=False,
    )
```

```python
import functools
import math

import jax
import jax.numpy as jnp
import numpy as np
from jax import lax
from jax.experimental import pallas as pl
from jax.experimental.pallas import tpu as pltpu
from jax.sharding import PartitionSpec as P

ROWS = 32
COLS = 64
BINS = 1024
BEAMS = 512
FRAMES = 16
REPLICA = 8192
PERIOD = 2 * BINS
LOCAL_BINS = 32
TAPS = REPLICA // 128 + 1


def start_powers():
    table = np.zeros((32, 16), np.float64)
    for place in range(32):
        first = BINS // 2 + place * LOCAL_BINS
        for bit in range(5):
            angle = 2.0 * math.pi * ((first << bit) % PERIOD) / PERIOD
            table[place, 2 * bit] = math.cos(angle)
            table[place, 2 * bit + 1] = math.sin(angle)
    return table.reshape(-1).astype(np.float32)


def inverse_factors():
    n = np.arange(BINS)
    fine = np.exp(2j * np.pi * ((np.arange(32)[:, None] * n) % BINS) / BINS) / math.sqrt(BINS)
    source = np.arange(32)
    first = (source % 4) * 256 + (source // 4) * 32
    coarse = np.exp(2j * np.pi * ((first[:, None] * n) % BINS) / BINS)
    return tuple(part.astype(np.float32) for part in (fine.real, fine.imag, coarse.real, coarse.imag))


def steer(lags, powers, factor):
    re, im = None, None
    for bit in range(5):
        pr, pi = powers[bit]
        chosen = (lags & (1 << bit)) != 0
        if re is None:
            re = jnp.where(chosen, pr * factor, jnp.full(lags.shape, factor, jnp.float32))
            im = jnp.where(chosen, pi * factor, jnp.zeros(lags.shape, jnp.float32))
        else:
            moved_re = re * pr - im * pi
            moved_im = re * pi + im * pr
            re = jnp.where(chosen, moved_re, re)
            im = jnp.where(chosen, moved_im, im)
    return re, im


def begin_steering(place, powers_ref, col_lags_ref, row_lags_ref, col, col_step, row, row_step):
    first = [
        (powers_ref[place * 16 + 2 * bit], powers_ref[place * 16 + 2 * bit + 1]) for bit in range(5)
    ]
    step = [
        (
            np.float32(math.cos(2.0 * math.pi * (1 << bit) / PERIOD)),
            np.float32(math.sin(2.0 * math.pi * (1 << bit) / PERIOD)),
        )
        for bit in range(5)
    ]
    for lags_ref, state, change, count, factor in (
        (col_lags_ref, col, col_step, COLS, COLS**-0.5),
        (row_lags_ref, row, row_step, ROWS, ROWS**-0.5),
    ):

        @pl.loop(0, count // 8)
        def _(group):
            rows = pl.ds(pl.multiple_of(group * 8, 8), 8)
            lags = lags_ref[rows, :]
            re, im = steer(lags, first, np.float32(factor))
            state[rows, 0:BEAMS] = re
            state[rows, BEAMS : 2 * BEAMS] = im
            re, im = steer(lags, step, np.float32(1.0))
            change[rows, 0:BEAMS] = re
            change[rows, BEAMS : 2 * BEAMS] = im


def advance(state, change, rows):
    re = state[rows, 0:BEAMS]
    im = state[rows, BEAMS : 2 * BEAMS]
    cr = change[rows, 0:BEAMS]
    ci = change[rows, BEAMS : 2 * BEAMS]
    state[rows, 0:BEAMS] = re * cr - im * ci
    state[rows, BEAMS : 2 * BEAMS] = re * ci + im * cr
    return re, im


def arrange_sensors(arrived, sensors):
    low = lax.broadcasted_iota(jnp.int32, (LOCAL_BINS, 128), 1) < 64
    for source in range(8):
        for pair in range(2):
            cols = slice(128 * pair, 128 * pair + 128)
            re = arrived[source, 0, :, cols].astype(jnp.float32)
            im = arrived[source, 1, :, cols].astype(jnp.float32)
            row = source * 4 + pair * 2
            sensors[row * 32 : row * 32 + 32, :] = jnp.where(low, re, pltpu.roll(im, 64, 1))
            row = row + 1
            sensors[row * 32 : row * 32 + 32, :] = jnp.where(low, pltpu.roll(re, 64, 1), im)


def build_steering(col, col_step, row, row_step, weights, row_table):
    @pl.loop(0, LOCAL_BINS)
    def _(bin_at):
        for group in range(COLS // 16):
            rows = slice(16 * group, 16 * group + 16)
            re, im = advance(col, col_step, rows)
            weights[bin_at, rows, 0:BEAMS] = re.astype(jnp.bfloat16)
            weights[bin_at, rows, BEAMS : 2 * BEAMS] = im.astype(jnp.bfloat16)
            rows = slice(64 + 16 * group, 64 + 16 * group + 16)
            weights[bin_at, rows, 0:BEAMS] = (-im).astype(jnp.bfloat16)
            weights[bin_at, rows, BEAMS : 2 * BEAMS] = re.astype(jnp.bfloat16)
        for group in range(ROWS // 8):
            rows = slice(8 * group, 8 * group + 8)
            re, im = advance(row, row_step, rows)
            row_table[bin_at, rows, 0:BEAMS] = re
            row_table[bin_at, rows, BEAMS : 2 * BEAMS] = im


def form_beams(sensors, weights, row_table, formed):
    formed[64:128, :] = jnp.zeros((64, BEAMS), jnp.float32)

    @pl.loop(0, LOCAL_BINS, unroll=4)
    def _(bin_at):
        data = sensors[pl.ds(bin_at, 32, stride=32), :].astype(jnp.bfloat16)
        along = jnp.dot(data, weights[bin_at], preferred_element_type=jnp.float32)
        row_re = row_table[bin_at, :, 0:BEAMS]
        row_im = row_table[bin_at, :, BEAMS : 2 * BEAMS]
        along_re = along[:, 0:BEAMS]
        along_im = along[:, BEAMS:]
        formed[pl.ds(bin_at, 1), :] = jnp.sum(along_re * row_re - along_im * row_im, axis=0, keepdims=True)
        formed[pl.ds(32 + bin_at, 1), :] = jnp.sum(along_re * row_im + along_im * row_re, axis=0, keepdims=True)


def pack_groups(formed, groups):
    low = lax.broadcasted_iota(jnp.int32, (8, 128), 1) < 64

    @pl.loop(0, 4)
    def _(quarter):
        turned = formed[:, pl.ds(pl.multiple_of(128 * quarter, 128), 128)].T
        for member in range(8):
            first = turned[16 * member : 16 * member + 8]
            second = turned[16 * member + 8 : 16 * member + 16]
            packed = jnp.where(low, first, pltpu.roll(second, 64, 1))
            groups[8 * quarter + member] = packed.astype(jnp.bfloat16)


def pack_beams(arrived, work, beams):
    low = lax.broadcasted_iota(jnp.int32, (8, 128), 1) < 64
    for pair in range(16):
        first = arrived[2 * pair].astype(jnp.float32)
        second = arrived[2 * pair + 1].astype(jnp.float32)
        work[8 * pair : 8 * pair + 8, :] = jnp.where(low, first, pltpu.roll(second, 64, 1))
        work[128 + 8 * pair : 136 + 8 * pair, :] = jnp.where(low, pltpu.roll(first, 64, 1), second)
    for beam in range(16):
        start = 128 * (beam // 8) + beam % 8
        beams[beam] = work[pl.ds(start, 16, stride=8), :].astype(jnp.bfloat16)


def gather_frames(arrived, work, gathered):
    for frame in range(FRAMES):
        work[16 * frame : 16 * frame + 16, :] = arrived[frame].astype(jnp.float32)
    for pair in range(16):
        gathered[:, 128 * pair : 128 * pair + 128] = work[pl.ds(pair, 16, stride=16), :].astype(jnp.bfloat16)


def lay_pulse(replica, length, lines, mirrored):
    lines[...] = jnp.zeros_like(lines)
    lane = lax.broadcasted_iota(jnp.int32, (2, 128), 1)
    for tap in range(TAPS - 1):
        line = replica[:, 128 * tap : 128 * tap + 128].astype(jnp.float32)
        lines[2 + 2 * tap : 4 + 2 * tap, :] = jnp.where(lane + 128 * tap < length, line, 0.0)
    down = lax.broadcasted_iota(jnp.int32, (128, 128), 0)
    across = lax.broadcasted_iota(jnp.int32, (128, 128), 1)
    turn = jnp.where((down + across) % 128 == 0, 1.0, 0.0).astype(jnp.bfloat16)
    mirrored[...] = jnp.dot(lines[...].astype(jnp.bfloat16), turn, preferred_element_type=jnp.float32)


def build_toeplitz(mirrored, toeplitz):
    down = lax.broadcasted_iota(jnp.int32, (128, 128), 0)
    across = lax.broadcasted_iota(jnp.int32, (128, 128), 1)
    lower = down >= across

    def circulant(row):
        line = jnp.broadcast_to(mirrored[pl.ds(row, 1), :], (128, 128))
        return pltpu.roll(line, 0, 1, stride=1, stride_axis=0)

    for part in range(2):

        @functools.partial(lax.fori_loop, 0, TAPS, init_val=circulant(part))
        def _(tap, before):
            rows = pl.ds(pl.multiple_of(tap * 128, 128), 128)
            here = circulant(2 * tap + 2 + part)
            toeplitz[rows, 128 * part : 128 * part + 128] = jnp.where(lower, here, before).astype(jnp.bfloat16)
            return here


def build_inverse(fine_re_ref, fine_im_ref, coarse_re_ref, coarse_im_ref, table):
    @pl.loop(0, 32)
    def _(source):
        start = pl.multiple_of(source * 64, 64)
        for half in range(2):
            for block in range(4):
                cols = slice(256 * block, 256 * block + 256)
                fr = fine_re_ref[16 * half : 16 * half + 16, cols]
                fi = fine_im_ref[16 * half : 16 * half + 16, cols]
                cr = coarse_re_ref[pl.ds(source, 1), cols]
                ci = coarse_im_ref[pl.ds(source, 1), cols]
                re = fr * cr - fi * ci
                im = fr * ci + fi * cr
                rows = pl.ds(start + 16 * half, 16)
                table[rows, cols] = re.astype(jnp.bfloat16)
                table[rows, slice(1024 + 256 * block, 1280 + 256 * block)] = im.astype(jnp.bfloat16)
                rows = pl.ds(start + 32 + 16 * half, 16)
                table[rows, cols] = (-im).astype(jnp.bfloat16)
                table[rows, slice(1024 + 256 * block, 1280 + 256 * block)] = re.astype(jnp.bfloat16)


def invert(gathered, table, series):
    series[...] = jnp.zeros_like(series)

    @pl.loop(0, 8)
    def _(block):
        cols = pl.ds(pl.multiple_of(256 * block, 256), 256)
        total = jnp.dot(gathered[...], table[:, cols], preferred_element_type=jnp.float32)
        for side in range(2):
            series[block // 4, 2 * (block % 4) + side, 0:16, :] = total[:, 128 * side : 128 * side + 128]


def spread(series, blocks):
    for part in range(2):
        for index in range(72):
            ahead, block = index // 8, index % 8
            blocks[part, 16 * index : 16 * index + 16, :] = series[part, block, ahead : ahead + 16, :].astype(
                jnp.bfloat16
            )


def correlate(blocks, toeplitz, total):
    def lines(tap):
        return jnp.concatenate(
            [blocks[part, pl.ds(pl.multiple_of(tap * 16, 16), 128), :] for part in range(2)], axis=0
        )

    last = TAPS - 1
    total[...] = jnp.dot(lines(last), toeplitz[128 * last : 128 * TAPS, :], preferred_element_type=jnp.float32)

    @pl.loop(0, last // 8)
    def _(group):
        tap = group * 8
        data = jnp.concatenate([lines(tap + member) for member in range(8)], axis=1)
        weights = toeplitz[pl.ds(pl.multiple_of(tap * 128, 1024), 1024), :]
        total[...] += jnp.dot(data, weights, preferred_element_type=jnp.float32)


def pack_echoes(total, work, leaving):
    for block in range(8):
        rows = slice(16 * block, 16 * block + 16)
        after = slice(128 + 16 * block, 144 + 16 * block)
        work[pl.ds(2 * block, 16, stride=16), :] = total[rows, 0:128] + total[after, 128:256]
        work[pl.ds(2 * block + 1, 16, stride=16), :] = total[after, 0:128] - total[rows, 128:256]
    for frame in range(FRAMES):
        leaving[frame] = work[16 * frame : 16 * frame + 16, :].astype(jnp.bfloat16)


def unpack_echoes(returned, work):
    for beam in range(16):
        work[16 * beam : 16 * beam + 16, :] = returned[beam].astype(jnp.float32)


RING8 = (4, 3, 5, 2, 6, 1, 7, 0)
RING4 = (2, 1, 3, 0)


def send(source, target, sends, receives, slot, device):
    return pltpu.make_async_remote_copy(
        src_ref=source,
        dst_ref=target,
        send_sem=sends.at[slot],
        recv_sem=receives.at[slot],
        device_id=device,
        device_id_type=pl.DeviceIdType.MESH,
    )


def ping_kernel(
    powers_ref,
    length_ref,
    spectra_hbm,
    col_lags_hbm,
    row_lags_hbm,
    replica_hbm,
    factors_hbm,
    out_hbm,
    spectra,
    col_lags,
    row_lags,
    replica,
    factors,
    arrived_bins,
    col,
    col_step,
    row,
    row_step,
    weights,
    row_table,
    sensors,
    formed,
    groups,
    arrived_groups,
    work,
    beams,
    arrived_beams,
    gathered,
    lines,
    mirrored,
    toeplitz,
    table,
    series,
    blocks,
    total,
    leaving,
    returned,
    local_sem,
    bin_send,
    bin_recv,
    group_send,
    group_recv,
    beam_send,
    beam_recv,
    out_send,
    out_recv,
):
    hyd = lax.axis_index("hyd")
    freq = lax.axis_index("freq")
    tm = lax.axis_index("tm")
    owner = hyd * 4 + freq

    inputs = [
        pltpu.make_async_copy(source, target, local_sem.at[index])
        for index, (source, target) in enumerate(
            (
                (spectra_hbm.at[:, 0], spectra),
                (col_lags_hbm, col_lags),
                (row_lags_hbm, row_lags),
                (replica_hbm, replica),
                (factors_hbm, factors),
            )
        )
    ]
    inputs[0].start()

    owners = []
    for ahead in RING8:
        for side in range(4):
            if ahead or side:
                to = ((hyd + ahead) & 7, (freq + side) & 3)
                back = ((hyd - ahead) & 7, (freq - side) & 3)
                owners.append((ahead * 4 + side, to[0] * 4 + to[1], back[0] * 4 + back[1], {"hyd": to[0], "freq": to[1]}))
    frames = []
    for far in RING4:
        for near in RING4:
            if far or near:
                to = ((((tm >> 2) + far) & 3) * 4) + ((tm + near) & 3)
                back = ((((tm >> 2) - far) & 3) * 4) + ((tm - near) & 3)
                frames.append((far * 4 + near, to, back, {"tm": to}))

    barrier = pltpu.get_barrier_semaphore()
    for _, _, _, device in owners + frames:
        pl.semaphore_signal(barrier, inc=1, device_id=device, device_id_type=pl.DeviceIdType.MESH)

    for copy in inputs[1:]:
        copy.start()
    inputs[0].wait()
    pl.semaphore_wait(barrier, 46)

    def bins_of(place):
        return spectra.at[:, pl.ds(pl.multiple_of(place * LOCAL_BINS, LOCAL_BINS), LOCAL_BINS), :]

    def bin_copy(ahead, source):
        place = (hyd + ahead) & 7
        return send(bins_of(place), arrived_bins.at[source], bin_send, bin_recv, ahead, {"hyd": place})

    for ahead in RING8[:-1]:
        bin_copy(ahead, hyd).start()
    own = pltpu.make_async_copy(bins_of(hyd), arrived_bins.at[hyd], local_sem.at[5])
    own.start()

    inputs[1].wait()
    inputs[2].wait()
    begin_steering(freq * 8 + hyd, powers_ref, col_lags, row_lags, col, col_step, row, row_step)
    build_steering(col, col_step, row, row_step, weights, row_table)
    inputs[3].wait()
    inputs[4].wait()
    lay_pulse(replica, length_ref[0], lines, mirrored)
    build_toeplitz(mirrored, toeplitz)
    build_inverse(factors.at[0], factors.at[1], factors.at[2], factors.at[3], table)

    own.wait()
    for ahead in RING8[-2::-1]:
        bin_copy(ahead, (hyd - ahead) & 7).wait_recv()
    arrange_sensors(arrived_bins, sensors)
    form_beams(sensors, weights, row_table, formed)
    pack_groups(formed, groups)

    def exchange(peers, mine, leaves, arrives, sends, receives):
        def copy(slot, place, source, device):
            return send(leaves.at[place], arrives.at[source], sends, receives, slot, device)

        for slot, place, _, device in peers:
            copy(slot, place, mine, device).start()
        own = pltpu.make_async_copy(leaves.at[mine], arrives.at[mine], local_sem.at[5])
        own.start()
        own.wait()
        for slot, place, source, device in peers[::-1]:
            copy(slot, place, source, device).wait_recv()

    def drain(peers, mine, leaves, arrives, sends, receives):
        for slot, place, _, device in peers:
            send(leaves.at[place], arrives.at[mine], sends, receives, slot, device).wait_send()

    exchange(owners, owner, groups, arrived_groups, group_send, group_recv)
    pack_beams(arrived_groups, work, beams)
    exchange(frames, tm, beams, arrived_beams, beam_send, beam_recv)
    gather_frames(arrived_beams, work, gathered)
    invert(gathered, table, series)
    spread(series, blocks)
    correlate(blocks, toeplitz, total)
    pack_echoes(total, work, leaving)
    exchange(frames, tm, leaving, returned, out_send, out_recv)
    unpack_echoes(returned, work)

    done = pltpu.make_async_copy(work, out_hbm, local_sem.at[5])
    done.start()
    for ahead in RING8[:-1]:
        bin_copy(ahead, hyd).wait_send()
    drain(owners, owner, groups, arrived_groups, group_send, group_recv)
    drain(frames, tm, beams, arrived_beams, beam_send, beam_recv)
    drain(frames, tm, leaving, returned, out_send, out_recv)
    done.wait()


def ping(spectra, row_lags, col_lags, replica, rep_len):
    factors = jnp.asarray(np.stack(inverse_factors()))
    smem = pl.BlockSpec(memory_space=pltpu.SMEM)
    hbm = pl.BlockSpec(memory_space=pl.ANY)
    bf16, f32, i32 = jnp.bfloat16, jnp.float32, jnp.int32
    dma = pltpu.SemaphoreType.DMA
    return pl.pallas_call(
        ping_kernel,
        out_shape=jax.ShapeDtypeStruct((256, 128), f32),
        in_specs=[smem, smem] + [hbm] * 5,
        out_specs=hbm,
        scratch_shapes=[
            pltpu.VMEM((2, 256, 256), bf16),
            pltpu.VMEM((COLS, BEAMS), i32),
            pltpu.VMEM((ROWS, BEAMS), i32),
            pltpu.VMEM((2, REPLICA), bf16),
            pltpu.VMEM((4, 32, BINS), f32),
            pltpu.VMEM((8, 2, LOCAL_BINS, 256), bf16),
            pltpu.VMEM((COLS, 2 * BEAMS), f32),
            pltpu.VMEM((COLS, 2 * BEAMS), f32),
            pltpu.VMEM((ROWS, 2 * BEAMS), f32),
            pltpu.VMEM((ROWS, 2 * BEAMS), f32),
            pltpu.VMEM((LOCAL_BINS, 128, 2 * BEAMS), bf16),
            pltpu.VMEM((LOCAL_BINS, ROWS, 2 * BEAMS), f32),
            pltpu.VMEM((1024, 128), f32),
            pltpu.VMEM((128, BEAMS), f32),
            pltpu.VMEM((32, 8, 128), bf16),
            pltpu.VMEM((32, 8, 128), bf16),
            pltpu.VMEM((256, 128), f32),
            pltpu.VMEM((16, 16, 128), bf16),
            pltpu.VMEM((16, 16, 128), bf16),
            pltpu.VMEM((16, 2048), bf16),
            pltpu.VMEM((144, 128), f32),
            pltpu.VMEM((144, 128), f32),
            pltpu.VMEM((TAPS * 128, 256), bf16),
            pltpu.VMEM((2048, 2048), bf16),
            pltpu.VMEM((2, 8, 24, 128), f32),
            pltpu.VMEM((2, 72 * 16, 128), bf16),
            pltpu.VMEM((256, 256), f32),
            pltpu.VMEM((16, 16, 128), bf16),
            pltpu.VMEM((16, 16, 128), bf16),
            dma((6,)),
            dma((8,)),
            dma((8,)),
            dma((32,)),
            dma((32,)),
            dma((16,)),
            dma((16,)),
            dma((16,)),
            dma((16,)),
        ],
        compiler_params=pltpu.CompilerParams(
            collective_id=0, has_side_effects=True, vmem_limit_bytes=60 * 1024 * 1024
        ),
    )(jnp.asarray(start_powers()), rep_len, spectra, col_lags, row_lags, replica, factors)


def on_device(spectra, row_lags, col_lags, replica, rep_len):
    returned = ping(spectra, row_lags, col_lags, replica, rep_len)
    return jnp.transpose(returned.reshape(16, 8, 2, 128), (0, 2, 1, 3)).reshape(16, 2, BINS)


def solution(mesh):
    placed = (P(None, "tm", "freq", "hyd"), P(), P(), P(), P())
    return jax.shard_map(
        on_device,
        mesh=mesh,
        in_specs=placed,
        out_specs=P(("hyd", "freq"), None, "tm"),
        check_vma=False,
    )
```

```python
import functools
import math

import jax
import jax.numpy as jnp
import numpy as np
from jax import lax
from jax.experimental import pallas as pl
from jax.experimental.pallas import tpu as pltpu
from jax.sharding import PartitionSpec as P

ROWS = 32
COLS = 64
BINS = 1024
BEAMS = 512
FRAMES = 16
REPLICA = 8192
PERIOD = 2 * BINS
LOCAL_BINS = 32
TAPS = REPLICA // 128 + 1


def start_powers():
    table = np.zeros((32, 16), np.float64)
    for place in range(32):
        first = BINS // 2 + place * LOCAL_BINS
        for bit in range(5):
            angle = 2.0 * math.pi * ((first << bit) % PERIOD) / PERIOD
            table[place, 2 * bit] = math.cos(angle)
            table[place, 2 * bit + 1] = math.sin(angle)
    return table.reshape(-1).astype(np.float32)


def inverse_factors():
    n = np.arange(BINS)
    fine = np.exp(2j * np.pi * ((np.arange(32)[:, None] * n) % BINS) / BINS) / math.sqrt(BINS)
    source = np.arange(32)
    first = (source % 4) * 256 + (source // 4) * 32
    coarse = np.exp(2j * np.pi * ((first[:, None] * n) % BINS) / BINS)
    return tuple(part.astype(np.float32) for part in (fine.real, fine.imag, coarse.real, coarse.imag))


def steer(lags, powers, factor):
    re, im = None, None
    for bit in range(5):
        pr, pi = powers[bit]
        chosen = (lags & (1 << bit)) != 0
        if re is None:
            re = jnp.where(chosen, pr * factor, jnp.full(lags.shape, factor, jnp.float32))
            im = jnp.where(chosen, pi * factor, jnp.zeros(lags.shape, jnp.float32))
        else:
            moved_re = re * pr - im * pi
            moved_im = re * pi + im * pr
            re = jnp.where(chosen, moved_re, re)
            im = jnp.where(chosen, moved_im, im)
    return re, im


def begin_steering(place, powers_ref, col_lags_ref, row_lags_ref, col, col_step, row, row_step):
    first = [
        (powers_ref[place * 16 + 2 * bit], powers_ref[place * 16 + 2 * bit + 1]) for bit in range(5)
    ]
    step = [
        (
            np.float32(math.cos(2.0 * math.pi * (1 << bit) / PERIOD)),
            np.float32(math.sin(2.0 * math.pi * (1 << bit) / PERIOD)),
        )
        for bit in range(5)
    ]
    for lags_ref, state, change, count, factor in (
        (col_lags_ref, col, col_step, COLS, COLS**-0.5),
        (row_lags_ref, row, row_step, ROWS, ROWS**-0.5),
    ):

        @pl.loop(0, count // 8)
        def _(group):
            rows = pl.ds(pl.multiple_of(group * 8, 8), 8)
            lags = lags_ref[rows, :]
            re, im = steer(lags, first, np.float32(factor))
            state[rows, 0:BEAMS] = re
            state[rows, BEAMS : 2 * BEAMS] = im
            re, im = steer(lags, step, np.float32(1.0))
            change[rows, 0:BEAMS] = re
            change[rows, BEAMS : 2 * BEAMS] = im


def advance(state, change, rows):
    re = state[rows, 0:BEAMS]
    im = state[rows, BEAMS : 2 * BEAMS]
    cr = change[rows, 0:BEAMS]
    ci = change[rows, BEAMS : 2 * BEAMS]
    state[rows, 0:BEAMS] = re * cr - im * ci
    state[rows, BEAMS : 2 * BEAMS] = re * ci + im * cr
    return re, im


def arrange_sensors(arrived, sensors):
    low = lax.broadcasted_iota(jnp.int32, (LOCAL_BINS, 128), 1) < 64
    for source in range(8):
        for pair in range(2):
            cols = slice(128 * pair, 128 * pair + 128)
            re = arrived[source, 0, :, cols].astype(jnp.float32)
            im = arrived[source, 1, :, cols].astype(jnp.float32)
            row = source * 4 + pair * 2
            sensors[row * 32 : row * 32 + 32, :] = jnp.where(low, re, pltpu.roll(im, 64, 1))
            row = row + 1
            sensors[row * 32 : row * 32 + 32, :] = jnp.where(low, pltpu.roll(re, 64, 1), im)


def build_steering(col, col_step, row, row_step, weights, row_table):
    @pl.loop(0, LOCAL_BINS)
    def _(bin_at):
        for group in range(COLS // 16):
            rows = slice(16 * group, 16 * group + 16)
            re, im = advance(col, col_step, rows)
            weights[bin_at, rows, 0:BEAMS] = re.astype(jnp.bfloat16)
            weights[bin_at, rows, BEAMS : 2 * BEAMS] = im.astype(jnp.bfloat16)
            rows = slice(64 + 16 * group, 64 + 16 * group + 16)
            weights[bin_at, rows, 0:BEAMS] = (-im).astype(jnp.bfloat16)
            weights[bin_at, rows, BEAMS : 2 * BEAMS] = re.astype(jnp.bfloat16)
        for group in range(ROWS // 8):
            rows = slice(8 * group, 8 * group + 8)
            re, im = advance(row, row_step, rows)
            row_table[bin_at, rows, 0:BEAMS] = re
            row_table[bin_at, rows, BEAMS : 2 * BEAMS] = im


def form_beams(sensors, weights, row_table, formed):
    formed[64:128, :] = jnp.zeros((64, BEAMS), jnp.float32)

    @pl.loop(0, LOCAL_BINS, unroll=4)
    def _(bin_at):
        data = sensors[pl.ds(bin_at, 32, stride=32), :].astype(jnp.bfloat16)
        along = jnp.dot(data, weights[bin_at], preferred_element_type=jnp.float32)
        row_re = row_table[bin_at, :, 0:BEAMS]
        row_im = row_table[bin_at, :, BEAMS : 2 * BEAMS]
        along_re = along[:, 0:BEAMS]
        along_im = along[:, BEAMS:]
        formed[pl.ds(bin_at, 1), :] = jnp.sum(along_re * row_re - along_im * row_im, axis=0, keepdims=True)
        formed[pl.ds(32 + bin_at, 1), :] = jnp.sum(along_re * row_im + along_im * row_re, axis=0, keepdims=True)


def pack_groups(formed, groups):
    low = lax.broadcasted_iota(jnp.int32, (8, 128), 1) < 64

    @pl.loop(0, 4)
    def _(quarter):
        turned = formed[:, pl.ds(pl.multiple_of(128 * quarter, 128), 128)].T
        for member in range(8):
            first = turned[16 * member : 16 * member + 8]
            second = turned[16 * member + 8 : 16 * member + 16]
            packed = jnp.where(low, first, pltpu.roll(second, 64, 1))
            groups[8 * quarter + member] = packed.astype(jnp.bfloat16)


def pack_beams(arrived, work, beams):
    low = lax.broadcasted_iota(jnp.int32, (8, 128), 1) < 64
    for pair in range(16):
        first = arrived[2 * pair].astype(jnp.float32)
        second = arrived[2 * pair + 1].astype(jnp.float32)
        work[8 * pair : 8 * pair + 8, :] = jnp.where(low, first, pltpu.roll(second, 64, 1))
        work[128 + 8 * pair : 136 + 8 * pair, :] = jnp.where(low, pltpu.roll(first, 64, 1), second)
    for beam in range(16):
        start = 128 * (beam // 8) + beam % 8
        beams[beam] = work[pl.ds(start, 16, stride=8), :].astype(jnp.bfloat16)


def gather_frames(arrived, work, gathered):
    for frame in range(FRAMES):
        work[16 * frame : 16 * frame + 16, :] = arrived[frame].astype(jnp.float32)
    for pair in range(16):
        gathered[:, 128 * pair : 128 * pair + 128] = work[pl.ds(pair, 16, stride=16), :].astype(jnp.bfloat16)


def lay_pulse(replica, length, lines, mirrored):
    lines[...] = jnp.zeros_like(lines)
    lane = lax.broadcasted_iota(jnp.int32, (2, 128), 1)
    for tap in range(TAPS - 1):
        line = replica[:, 128 * tap : 128 * tap + 128].astype(jnp.float32)
        lines[2 + 2 * tap : 4 + 2 * tap, :] = jnp.where(lane + 128 * tap < length, line, 0.0)
    down = lax.broadcasted_iota(jnp.int32, (128, 128), 0)
    across = lax.broadcasted_iota(jnp.int32, (128, 128), 1)
    turn = jnp.where((down + across) % 128 == 0, 1.0, 0.0).astype(jnp.bfloat16)
    mirrored[...] = jnp.dot(lines[...].astype(jnp.bfloat16), turn, preferred_element_type=jnp.float32)


def build_toeplitz(mirrored, toeplitz):
    down = lax.broadcasted_iota(jnp.int32, (128, 128), 0)
    across = lax.broadcasted_iota(jnp.int32, (128, 128), 1)
    lower = down >= across

    @pl.loop(0, TAPS // 5)
    def _(group):
        for part in range(2):
            turned = []
            for member in range(6):
                line = mirrored[pl.ds(2 * (group * 5 + member) + part, 1), :]
                turned.append(pltpu.roll(jnp.broadcast_to(line, (128, 128)), 0, 1, stride=1, stride_axis=0))
            for member in range(5):
                rows = pl.ds(pl.multiple_of((group * 5 + member) * 128, 128), 128)
                both = jnp.where(lower, turned[member + 1], turned[member])
                toeplitz[rows, 128 * part : 128 * part + 128] = both.astype(jnp.bfloat16)


def build_inverse(fine_re_ref, fine_im_ref, coarse_re_ref, coarse_im_ref, table):
    @pl.loop(0, 32)
    def _(source):
        start = pl.multiple_of(source * 64, 64)
        for half in range(2):
            for block in range(4):
                cols = slice(256 * block, 256 * block + 256)
                fr = fine_re_ref[16 * half : 16 * half + 16, cols]
                fi = fine_im_ref[16 * half : 16 * half + 16, cols]
                cr = coarse_re_ref[pl.ds(source, 1), cols]
                ci = coarse_im_ref[pl.ds(source, 1), cols]
                re = fr * cr - fi * ci
                im = fr * ci + fi * cr
                rows = pl.ds(start + 16 * half, 16)
                table[rows, cols] = re.astype(jnp.bfloat16)
                table[rows, slice(1024 + 256 * block, 1280 + 256 * block)] = im.astype(jnp.bfloat16)
                rows = pl.ds(start + 32 + 16 * half, 16)
                table[rows, cols] = (-im).astype(jnp.bfloat16)
                table[rows, slice(1024 + 256 * block, 1280 + 256 * block)] = re.astype(jnp.bfloat16)


def invert(gathered, table, series):
    series[...] = jnp.zeros_like(series)

    @pl.loop(0, 4)
    def _(block):
        cols = pl.ds(pl.multiple_of(512 * block, 512), 512)
        total = jnp.dot(gathered[...], table[:, cols], preferred_element_type=jnp.float32)
        for side in range(4):
            series[block // 2, 4 * (block % 2) + side, 0:16, :] = total[:, 128 * side : 128 * side + 128]


def spread(series, blocks):
    for part in range(2):
        for index in range(72):
            ahead, block = index // 8, index % 8
            blocks[part, 16 * index : 16 * index + 16, :] = series[part, block, ahead : ahead + 16, :].astype(
                jnp.bfloat16
            )


def correlate(blocks, toeplitz, total):
    def lines(tap):
        return jnp.concatenate(
            [blocks[part, pl.ds(pl.multiple_of(tap * 16, 16), 128), :] for part in range(2)], axis=0
        )

    last = TAPS - 1
    total[...] = jnp.dot(lines(last), toeplitz[128 * last : 128 * TAPS, :], preferred_element_type=jnp.float32)

    @pl.loop(0, last // 16)
    def _(group):
        tap = group * 16
        data = jnp.concatenate([lines(tap + member) for member in range(16)], axis=1)
        weights = toeplitz[pl.ds(pl.multiple_of(tap * 128, 16 * 128), 16 * 128), :]
        total[...] += jnp.dot(data, weights, preferred_element_type=jnp.float32)


def pack_echoes(total, work, leaving):
    for block in range(8):
        rows = slice(16 * block, 16 * block + 16)
        after = slice(128 + 16 * block, 144 + 16 * block)
        work[pl.ds(2 * block, 16, stride=16), :] = total[rows, 0:128] + total[after, 128:256]
        work[pl.ds(2 * block + 1, 16, stride=16), :] = total[after, 0:128] - total[rows, 128:256]
    for frame in range(FRAMES):
        leaving[frame] = work[16 * frame : 16 * frame + 16, :].astype(jnp.bfloat16)


def unpack_echoes(returned, work):
    for beam in range(16):
        work[16 * beam : 16 * beam + 16, :] = returned[beam].astype(jnp.float32)


RING8 = (4, 3, 5, 2, 6, 1, 7, 0)
RING4 = (2, 1, 3, 0)


def send(source, target, sends, receives, slot, device):
    return pltpu.make_async_remote_copy(
        src_ref=source,
        dst_ref=target,
        send_sem=sends.at[slot],
        recv_sem=receives.at[slot],
        device_id=device,
        device_id_type=pl.DeviceIdType.MESH,
    )


def ping_kernel(
    powers_ref,
    length_ref,
    spectra_hbm,
    col_lags_hbm,
    row_lags_hbm,
    replica_hbm,
    factors_hbm,
    out_hbm,
    spectra,
    col_lags,
    row_lags,
    replica,
    factors,
    arrived_bins,
    col,
    col_step,
    row,
    row_step,
    weights,
    row_table,
    sensors,
    formed,
    groups,
    arrived_groups,
    work,
    beams,
    arrived_beams,
    gathered,
    lines,
    mirrored,
    toeplitz,
    table,
    series,
    blocks,
    total,
    leaving,
    returned,
    local_sem,
    bin_send,
    bin_recv,
    group_send,
    group_recv,
    beam_send,
    beam_recv,
    out_send,
    out_recv,
):
    hyd = lax.axis_index("hyd")
    freq = lax.axis_index("freq")
    tm = lax.axis_index("tm")
    owner = hyd * 4 + freq

    inputs = [
        pltpu.make_async_copy(source, target, local_sem.at[index])
        for index, (source, target) in enumerate(
            (
                (spectra_hbm.at[:, 0], spectra),
                (col_lags_hbm, col_lags),
                (row_lags_hbm, row_lags),
                (replica_hbm, replica),
                (factors_hbm, factors),
            )
        )
    ]
    inputs[0].start()

    owners = []
    for ahead in RING8:
        for side in range(4):
            if ahead or side:
                to = ((hyd + ahead) & 7, (freq + side) & 3)
                back = ((hyd - ahead) & 7, (freq - side) & 3)
                owners.append((ahead * 4 + side, to[0] * 4 + to[1], back[0] * 4 + back[1], {"hyd": to[0], "freq": to[1]}))
    frames = []
    for far in RING4:
        for near in RING4:
            if far or near:
                to = ((((tm >> 2) + far) & 3) * 4) + ((tm + near) & 3)
                back = ((((tm >> 2) - far) & 3) * 4) + ((tm - near) & 3)
                frames.append((far * 4 + near, to, back, {"tm": to}))

    barrier = pltpu.get_barrier_semaphore()
    for _, _, _, device in owners + frames:
        pl.semaphore_signal(barrier, inc=1, device_id=device, device_id_type=pl.DeviceIdType.MESH)

    for copy in inputs[1:]:
        copy.start()
    inputs[0].wait()
    pl.semaphore_wait(barrier, 46)

    def bins_of(place):
        return spectra.at[:, pl.ds(pl.multiple_of(place * LOCAL_BINS, LOCAL_BINS), LOCAL_BINS), :]

    def bin_copy(ahead, source):
        place = (hyd + ahead) & 7
        return send(bins_of(place), arrived_bins.at[source], bin_send, bin_recv, ahead, {"hyd": place})

    for ahead in RING8[:-1]:
        bin_copy(ahead, hyd).start()
    own = pltpu.make_async_copy(bins_of(hyd), arrived_bins.at[hyd], local_sem.at[5])
    own.start()

    inputs[1].wait()
    inputs[2].wait()
    begin_steering(freq * 8 + hyd, powers_ref, col_lags, row_lags, col, col_step, row, row_step)
    build_steering(col, col_step, row, row_step, weights, row_table)
    inputs[3].wait()
    inputs[4].wait()
    lay_pulse(replica, length_ref[0], lines, mirrored)
    build_toeplitz(mirrored, toeplitz)
    build_inverse(factors.at[0], factors.at[1], factors.at[2], factors.at[3], table)

    own.wait()
    for ahead in RING8[-2::-1]:
        bin_copy(ahead, (hyd - ahead) & 7).wait_recv()
    arrange_sensors(arrived_bins, sensors)
    form_beams(sensors, weights, row_table, formed)
    pack_groups(formed, groups)

    def exchange(peers, mine, leaves, arrives, sends, receives):
        def copy(slot, place, source, device):
            return send(leaves.at[place], arrives.at[source], sends, receives, slot, device)

        for slot, place, _, device in peers:
            copy(slot, place, mine, device).start()
        own = pltpu.make_async_copy(leaves.at[mine], arrives.at[mine], local_sem.at[5])
        own.start()
        own.wait()
        for slot, place, source, device in peers[::-1]:
            copy(slot, place, source, device).wait_recv()

    def drain(peers, mine, leaves, arrives, sends, receives):
        for slot, place, _, device in peers:
            send(leaves.at[place], arrives.at[mine], sends, receives, slot, device).wait_send()

    exchange(owners, owner, groups, arrived_groups, group_send, group_recv)
    pack_beams(arrived_groups, work, beams)
    exchange(frames, tm, beams, arrived_beams, beam_send, beam_recv)
    gather_frames(arrived_beams, work, gathered)
    invert(gathered, table, series)
    spread(series, blocks)
    correlate(blocks, toeplitz, total)
    pack_echoes(total, work, leaving)
    exchange(frames, tm, leaving, returned, out_send, out_recv)
    unpack_echoes(returned, work)

    done = pltpu.make_async_copy(work, out_hbm, local_sem.at[5])
    done.start()
    for ahead in RING8[:-1]:
        bin_copy(ahead, hyd).wait_send()
    drain(owners, owner, groups, arrived_groups, group_send, group_recv)
    drain(frames, tm, beams, arrived_beams, beam_send, beam_recv)
    drain(frames, tm, leaving, returned, out_send, out_recv)
    done.wait()


def ping(spectra, row_lags, col_lags, replica, rep_len):
    factors = jnp.asarray(np.stack(inverse_factors()))
    smem = pl.BlockSpec(memory_space=pltpu.SMEM)
    hbm = pl.BlockSpec(memory_space=pl.ANY)
    bf16, f32, i32 = jnp.bfloat16, jnp.float32, jnp.int32
    dma = pltpu.SemaphoreType.DMA
    return pl.pallas_call(
        ping_kernel,
        out_shape=jax.ShapeDtypeStruct((256, 128), f32),
        in_specs=[smem, smem] + [hbm] * 5,
        out_specs=hbm,
        scratch_shapes=[
            pltpu.VMEM((2, 256, 256), bf16),
            pltpu.VMEM((COLS, BEAMS), i32),
            pltpu.VMEM((ROWS, BEAMS), i32),
            pltpu.VMEM((2, REPLICA), bf16),
            pltpu.VMEM((4, 32, BINS), f32),
            pltpu.VMEM((8, 2, LOCAL_BINS, 256), bf16),
            pltpu.VMEM((COLS, 2 * BEAMS), f32),
            pltpu.VMEM((COLS, 2 * BEAMS), f32),
            pltpu.VMEM((ROWS, 2 * BEAMS), f32),
            pltpu.VMEM((ROWS, 2 * BEAMS), f32),
            pltpu.VMEM((LOCAL_BINS, 128, 2 * BEAMS), bf16),
            pltpu.VMEM((LOCAL_BINS, ROWS, 2 * BEAMS), f32),
            pltpu.VMEM((1024, 128), f32),
            pltpu.VMEM((128, BEAMS), f32),
            pltpu.VMEM((32, 8, 128), bf16),
            pltpu.VMEM((32, 8, 128), bf16),
            pltpu.VMEM((256, 128), f32),
            pltpu.VMEM((16, 16, 128), bf16),
            pltpu.VMEM((16, 16, 128), bf16),
            pltpu.VMEM((16, 2048), bf16),
            pltpu.VMEM((144, 128), f32),
            pltpu.VMEM((144, 128), f32),
            pltpu.VMEM((TAPS * 128, 256), bf16),
            pltpu.VMEM((2048, 2048), bf16),
            pltpu.VMEM((2, 8, 24, 128), f32),
            pltpu.VMEM((2, 72 * 16, 128), bf16),
            pltpu.VMEM((256, 256), f32),
            pltpu.VMEM((16, 16, 128), bf16),
            pltpu.VMEM((16, 16, 128), bf16),
            dma((6,)),
            dma((8,)),
            dma((8,)),
            dma((32,)),
            dma((32,)),
            dma((16,)),
            dma((16,)),
            dma((16,)),
            dma((16,)),
        ],
        compiler_params=pltpu.CompilerParams(
            collective_id=0, has_side_effects=True, vmem_limit_bytes=60 * 1024 * 1024
        ),
    )(jnp.asarray(start_powers()), rep_len, spectra, col_lags, row_lags, replica, factors)


def on_device(spectra, row_lags, col_lags, replica, rep_len):
    returned = ping(spectra, row_lags, col_lags, replica, rep_len)
    return jnp.transpose(returned.reshape(16, 8, 2, 128), (0, 2, 1, 3)).reshape(16, 2, BINS)


def solution(mesh):
    placed = (P(None, "tm", "freq", "hyd"), P(), P(), P(), P())
    return jax.shard_map(
        on_device,
        mesh=mesh,
        in_specs=placed,
        out_specs=P(("hyd", "freq"), None, "tm"),
        check_vma=False,
    )
```

```python
import functools
import math

import jax
import jax.numpy as jnp
import numpy as np
from jax import lax
from jax.experimental import pallas as pl
from jax.experimental.pallas import tpu as pltpu
from jax.sharding import PartitionSpec as P

ROWS = 32
COLS = 64
BINS = 1024
BEAMS = 512
FRAMES = 16
REPLICA = 8192
PERIOD = 2 * BINS
LOCAL_BINS = 32
HALF = LOCAL_BINS // 2
TAPS = REPLICA // 128 + 1


def start_powers():
    table = np.zeros((32, 16), np.float64)
    for place in range(32):
        first = BINS // 2 + place * LOCAL_BINS
        for bit in range(5):
            angle = 2.0 * math.pi * ((first << bit) % PERIOD) / PERIOD
            table[place, 2 * bit] = math.cos(angle)
            table[place, 2 * bit + 1] = math.sin(angle)
    return table.reshape(-1).astype(np.float32)


def inverse_factors():
    n = np.arange(BINS)
    fine = np.exp(2j * np.pi * ((np.arange(32)[:, None] * n) % BINS) / BINS) / math.sqrt(BINS)
    source = np.arange(32)
    first = (source % 4) * 256 + (source // 4) * 32
    coarse = np.exp(2j * np.pi * ((first[:, None] * n) % BINS) / BINS)
    return tuple(part.astype(np.float32) for part in (fine.real, fine.imag, coarse.real, coarse.imag))


def steer(lags, powers, factor):
    re, im = None, None
    for bit in range(5):
        pr, pi = powers[bit]
        chosen = (lags & (1 << bit)) != 0
        if re is None:
            re = jnp.where(chosen, pr * factor, jnp.full(lags.shape, factor, jnp.float32))
            im = jnp.where(chosen, pi * factor, jnp.zeros(lags.shape, jnp.float32))
        else:
            moved_re = re * pr - im * pi
            moved_im = re * pi + im * pr
            re = jnp.where(chosen, moved_re, re)
            im = jnp.where(chosen, moved_im, im)
    return re, im


def begin_steering(place, powers_ref, col_lags_ref, row_lags_ref, col, col_step, row, row_step):
    first = [
        (powers_ref[place * 16 + 2 * bit], powers_ref[place * 16 + 2 * bit + 1]) for bit in range(5)
    ]
    step = [
        (
            np.float32(math.cos(2.0 * math.pi * (1 << bit) / PERIOD)),
            np.float32(math.sin(2.0 * math.pi * (1 << bit) / PERIOD)),
        )
        for bit in range(5)
    ]
    for lags_ref, state, change, count, factor in (
        (col_lags_ref, col, col_step, COLS, COLS**-0.5),
        (row_lags_ref, row, row_step, ROWS, ROWS**-0.5),
    ):

        @pl.loop(0, count // 8)
        def _(group):
            rows = pl.ds(pl.multiple_of(group * 8, 8), 8)
            lags = lags_ref[rows, :]
            re, im = steer(lags, first, np.float32(factor))
            state[rows, 0:BEAMS] = re
            state[rows, BEAMS : 2 * BEAMS] = im
            re, im = steer(lags, step, np.float32(1.0))
            change[rows, 0:BEAMS] = re
            change[rows, BEAMS : 2 * BEAMS] = im


def advance(state, change, rows):
    re = state[rows, 0:BEAMS]
    im = state[rows, BEAMS : 2 * BEAMS]
    cr = change[rows, 0:BEAMS]
    ci = change[rows, BEAMS : 2 * BEAMS]
    state[rows, 0:BEAMS] = re * cr - im * ci
    state[rows, BEAMS : 2 * BEAMS] = re * ci + im * cr
    return re, im


def arrange_sensors(arrived, sensors, half):
    low = lax.broadcasted_iota(jnp.int32, (HALF, 128), 1) < 64
    bins = pl.ds(pl.multiple_of(half * HALF, HALF), HALF)
    for source in range(8):
        for pair in range(2):
            cols = slice(128 * pair, 128 * pair + 128)
            re = arrived[source, 0, bins, cols].astype(jnp.float32)
            im = arrived[source, 1, bins, cols].astype(jnp.float32)
            row = source * 4 + pair * 2
            start = pl.multiple_of(half * HALF, HALF)
            sensors[pl.ds(row * 32 + start, HALF), :] = jnp.where(low, re, pltpu.roll(im, 64, 1))
            sensors[pl.ds(row * 32 + 32 + start, HALF), :] = jnp.where(low, pltpu.roll(re, 64, 1), im)


def build_steering(col, col_step, row, row_step, weights, row_table):
    @pl.loop(0, LOCAL_BINS)
    def _(bin_at):
        for group in range(COLS // 16):
            rows = slice(16 * group, 16 * group + 16)
            re, im = advance(col, col_step, rows)
            weights[bin_at, rows, 0:BEAMS] = re.astype(jnp.bfloat16)
            weights[bin_at, rows, BEAMS : 2 * BEAMS] = im.astype(jnp.bfloat16)
            rows = slice(64 + 16 * group, 64 + 16 * group + 16)
            weights[bin_at, rows, 0:BEAMS] = (-im).astype(jnp.bfloat16)
            weights[bin_at, rows, BEAMS : 2 * BEAMS] = re.astype(jnp.bfloat16)
        for group in range(ROWS // 8):
            rows = slice(8 * group, 8 * group + 8)
            re, im = advance(row, row_step, rows)
            row_table[bin_at, rows, 0:BEAMS] = re
            row_table[bin_at, rows, BEAMS : 2 * BEAMS] = im


def form_beams(sensors, weights, row_table, formed, half):
    @pl.loop(0, HALF, unroll=4)
    def _(step):
        bin_at = half * HALF + step
        data = sensors[pl.ds(bin_at, 32, stride=32), :].astype(jnp.bfloat16)
        along = jnp.dot(data, weights[bin_at], preferred_element_type=jnp.float32)
        row_re = row_table[bin_at, :, 0:BEAMS]
        row_im = row_table[bin_at, :, BEAMS : 2 * BEAMS]
        along_re = along[:, 0:BEAMS]
        along_im = along[:, BEAMS:]
        formed[pl.ds(bin_at, 1), :] = jnp.sum(along_re * row_re - along_im * row_im, axis=0, keepdims=True)
        formed[pl.ds(32 + bin_at, 1), :] = jnp.sum(along_re * row_im + along_im * row_re, axis=0, keepdims=True)


def pack_groups(formed, groups):
    low = lax.broadcasted_iota(jnp.int32, (8, 128), 1) < 64

    @pl.loop(0, 4)
    def _(quarter):
        turned = formed[:, pl.ds(pl.multiple_of(128 * quarter, 128), 128)].T
        for member in range(8):
            first = turned[16 * member : 16 * member + 8]
            second = turned[16 * member + 8 : 16 * member + 16]
            packed = jnp.where(low, first, pltpu.roll(second, 64, 1))
            groups[8 * quarter + member] = packed.astype(jnp.bfloat16)


def pack_beams(arrived, work, beams):
    low = lax.broadcasted_iota(jnp.int32, (8, 128), 1) < 64
    for pair in range(16):
        first = arrived[2 * pair].astype(jnp.float32)
        second = arrived[2 * pair + 1].astype(jnp.float32)
        work[8 * pair : 8 * pair + 8, :] = jnp.where(low, first, pltpu.roll(second, 64, 1))
        work[128 + 8 * pair : 136 + 8 * pair, :] = jnp.where(low, pltpu.roll(first, 64, 1), second)
    for beam in range(16):
        start = 128 * (beam // 8) + beam % 8
        beams[beam] = work[pl.ds(start, 16, stride=8), :].astype(jnp.bfloat16)


def gather_frames(arrived, work, gathered):
    for frame in range(FRAMES):
        work[16 * frame : 16 * frame + 16, :] = arrived[frame].astype(jnp.float32)
    for pair in range(16):
        gathered[:, 128 * pair : 128 * pair + 128] = work[pl.ds(pair, 16, stride=16), :].astype(jnp.bfloat16)


def lay_pulse(replica, length, lines, mirrored):
    lines[...] = jnp.zeros_like(lines)
    lane = lax.broadcasted_iota(jnp.int32, (2, 128), 1)
    for tap in range(TAPS - 1):
        line = replica[:, 128 * tap : 128 * tap + 128].astype(jnp.float32)
        lines[2 + 2 * tap : 4 + 2 * tap, :] = jnp.where(lane + 128 * tap < length, line, 0.0)
    down = lax.broadcasted_iota(jnp.int32, (128, 128), 0)
    across = lax.broadcasted_iota(jnp.int32, (128, 128), 1)
    turn = jnp.where((down + across) % 128 == 0, 1.0, 0.0).astype(jnp.bfloat16)
    mirrored[...] = jnp.dot(lines[...].astype(jnp.bfloat16), turn, preferred_element_type=jnp.float32)


def build_toeplitz(mirrored, toeplitz):
    down = lax.broadcasted_iota(jnp.int32, (128, 128), 0)
    across = lax.broadcasted_iota(jnp.int32, (128, 128), 1)
    lower = down >= across

    @pl.loop(0, TAPS // 5)
    def _(group):
        for part in range(2):
            turned = []
            for member in range(6):
                line = mirrored[pl.ds(2 * (group * 5 + member) + part, 1), :]
                turned.append(pltpu.roll(jnp.broadcast_to(line, (128, 128)), 0, 1, stride=1, stride_axis=0))
            for member in range(5):
                rows = pl.ds(pl.multiple_of((group * 5 + member) * 128, 128), 128)
                both = jnp.where(lower, turned[member + 1], turned[member])
                toeplitz[rows, 128 * part : 128 * part + 128] = both.astype(jnp.bfloat16)


def build_inverse(fine_re_ref, fine_im_ref, coarse_re_ref, coarse_im_ref, table):
    @pl.loop(0, 32)
    def _(source):
        start = pl.multiple_of(source * 64, 64)
        for half in range(2):
            for block in range(4):
                cols = slice(256 * block, 256 * block + 256)
                fr = fine_re_ref[16 * half : 16 * half + 16, cols]
                fi = fine_im_ref[16 * half : 16 * half + 16, cols]
                cr = coarse_re_ref[pl.ds(source, 1), cols]
                ci = coarse_im_ref[pl.ds(source, 1), cols]
                re = fr * cr - fi * ci
                im = fr * ci + fi * cr
                rows = pl.ds(start + 16 * half, 16)
                table[rows, cols] = re.astype(jnp.bfloat16)
                table[rows, slice(1024 + 256 * block, 1280 + 256 * block)] = im.astype(jnp.bfloat16)
                rows = pl.ds(start + 32 + 16 * half, 16)
                table[rows, cols] = (-im).astype(jnp.bfloat16)
                table[rows, slice(1024 + 256 * block, 1280 + 256 * block)] = re.astype(jnp.bfloat16)


def invert(gathered, table, series):
    series[...] = jnp.zeros_like(series)

    @pl.loop(0, 4)
    def _(block):
        cols = pl.ds(pl.multiple_of(512 * block, 512), 512)
        total = jnp.dot(gathered[...], table[:, cols], preferred_element_type=jnp.float32)
        for side in range(4):
            series[block // 2, 4 * (block % 2) + side, 0:16, :] = total[:, 128 * side : 128 * side + 128]


def spread(series, blocks):
    for part in range(2):
        for index in range(72):
            ahead, block = index // 8, index % 8
            blocks[part, 16 * index : 16 * index + 16, :] = series[part, block, ahead : ahead + 16, :].astype(
                jnp.bfloat16
            )


def correlate(blocks, toeplitz, total):
    def lines(tap):
        return jnp.concatenate(
            [blocks[part, pl.ds(pl.multiple_of(tap * 16, 16), 128), :] for part in range(2)], axis=0
        )

    last = TAPS - 1
    total[...] = jnp.dot(lines(last), toeplitz[128 * last : 128 * TAPS, :], preferred_element_type=jnp.float32)

    @pl.loop(0, last // 16)
    def _(group):
        tap = group * 16
        data = jnp.concatenate([lines(tap + member) for member in range(16)], axis=1)
        weights = toeplitz[pl.ds(pl.multiple_of(tap * 128, 16 * 128), 16 * 128), :]
        total[...] += jnp.dot(data, weights, preferred_element_type=jnp.float32)


def pack_echoes(total, work, leaving):
    for block in range(8):
        rows = slice(16 * block, 16 * block + 16)
        after = slice(128 + 16 * block, 144 + 16 * block)
        work[pl.ds(2 * block, 16, stride=16), :] = total[rows, 0:128] + total[after, 128:256]
        work[pl.ds(2 * block + 1, 16, stride=16), :] = total[after, 0:128] - total[rows, 128:256]
    for frame in range(FRAMES):
        leaving[frame] = work[16 * frame : 16 * frame + 16, :].astype(jnp.bfloat16)


def unpack_echoes(returned, work):
    for beam in range(16):
        work[16 * beam : 16 * beam + 16, :] = returned[beam].astype(jnp.float32)


RING8 = (4, 3, 5, 2, 6, 1, 7, 0)
RING4 = (2, 1, 3, 0)


def send(source, target, sends, receives, slot, device):
    return pltpu.make_async_remote_copy(
        src_ref=source,
        dst_ref=target,
        send_sem=sends.at[slot],
        recv_sem=receives.at[slot],
        device_id=device,
        device_id_type=pl.DeviceIdType.MESH,
    )


def ping_kernel(
    powers_ref,
    length_ref,
    spectra_hbm,
    col_lags_hbm,
    row_lags_hbm,
    replica_hbm,
    factors_hbm,
    out_hbm,
    spectra,
    col_lags,
    row_lags,
    replica,
    factors,
    arrived_bins,
    col,
    col_step,
    row,
    row_step,
    weights,
    row_table,
    sensors,
    formed,
    groups,
    arrived_groups,
    work,
    beams,
    arrived_beams,
    gathered,
    lines,
    mirrored,
    toeplitz,
    table,
    series,
    blocks,
    total,
    leaving,
    returned,
    local_sem,
    bin_send,
    bin_recv,
    group_send,
    group_recv,
    beam_send,
    beam_recv,
    out_send,
    out_recv,
    relayed,
):
    hyd = lax.axis_index("hyd")
    freq = lax.axis_index("freq")
    tm = lax.axis_index("tm")
    owner = hyd * 4 + freq

    inputs = [
        pltpu.make_async_copy(source, target, local_sem.at[index])
        for index, (source, target) in enumerate(
            (
                (spectra_hbm.at[:, 0], spectra),
                (col_lags_hbm, col_lags),
                (row_lags_hbm, row_lags),
                (replica_hbm, replica),
                (factors_hbm, factors),
            )
        )
    ]
    inputs[0].start()

    owners = []
    for ahead in RING8:
        for side in range(4):
            if ahead or side:
                to = ((hyd + ahead) & 7, (freq + side) & 3)
                back = ((hyd - ahead) & 7, (freq - side) & 3)
                owners.append((ahead * 4 + side, to[0] * 4 + to[1], back[0] * 4 + back[1], {"hyd": to[0], "freq": to[1]}))
    frames = []
    for far in RING4:
        for near in RING4:
            if far or near:
                to = ((((tm >> 2) + far) & 3) * 4) + ((tm + near) & 3)
                back = ((((tm >> 2) - far) & 3) * 4) + ((tm - near) & 3)
                frames.append((far * 4 + near, to, back, {"tm": to}))

    barrier = pltpu.get_barrier_semaphore()
    beside = [{"freq": (freq + side) & 3} for side in range(1, 4)]
    near = [{"tm": (tm & 12) + ((tm + step) & 3)} for step in range(1, 4)]
    along = [{"hyd": (hyd + ahead) & 7} for ahead in RING8[:-1]]
    across = [{"tm": (tm + 4 * step) & 15} for step in range(1, 4)]
    for device in along + across + near + beside:
        pl.semaphore_signal(barrier, inc=1, device_id=device, device_id_type=pl.DeviceIdType.MESH)

    for copy in inputs[1:]:
        copy.start()
    inputs[0].wait()
    pl.semaphore_wait(barrier, 16)

    def bin_copy(half, ahead, source):
        place = (hyd + ahead) & 7
        start = pl.multiple_of(place * LOCAL_BINS + half * HALF, HALF)
        bins = pl.ds(pl.multiple_of(half * HALF, HALF), HALF)
        return send(
            spectra.at[:, pl.ds(start, HALF), :],
            arrived_bins.at[source, :, bins, :],
            bin_send,
            bin_recv,
            half * 8 + ahead,
            {"hyd": place},
        )

    for half in range(2):
        for ahead in RING8[:-1]:
            bin_copy(half, ahead, hyd).start()
    mine = pl.ds(pl.multiple_of(hyd * LOCAL_BINS, LOCAL_BINS), LOCAL_BINS)
    own = pltpu.make_async_copy(spectra.at[:, mine, :], arrived_bins.at[hyd], local_sem.at[5])
    own.start()
    for device in near + beside:
        pl.semaphore_signal(relayed, inc=1, device_id=device, device_id_type=pl.DeviceIdType.MESH)

    inputs[1].wait()
    inputs[2].wait()
    begin_steering(freq * 8 + hyd, powers_ref, col_lags, row_lags, col, col_step, row, row_step)
    build_steering(col, col_step, row, row_step, weights, row_table)
    inputs[3].wait()
    lay_pulse(replica, length_ref[0], lines, mirrored)
    formed[64:128, :] = jnp.zeros((64, BEAMS), jnp.float32)
    own.wait()

    @pl.loop(0, 2)
    def _(half):
        for ahead in RING8[-2::-1]:
            bin_copy(half, ahead, (hyd - ahead) & 7).wait_recv()
        arrange_sensors(arrived_bins, sensors, half)
        form_beams(sensors, weights, row_table, formed, half)

    pack_groups(formed, groups)
    pl.semaphore_wait(relayed, 6)

    def exchange(peers, mine, leaves, arrives, sends, receives, meanwhile=None):
        def copy(slot, place, source, device):
            return send(leaves.at[place], arrives.at[source], sends, receives, slot, device)

        for slot, place, _, device in peers:
            copy(slot, place, mine, device).start()
        own = pltpu.make_async_copy(leaves.at[mine], arrives.at[mine], local_sem.at[5])
        own.start()
        if meanwhile is not None:
            meanwhile()
        own.wait()
        for slot, place, source, device in peers[::-1]:
            copy(slot, place, source, device).wait_recv()

    def drain(peers, mine, leaves, arrives, sends, receives):
        for slot, place, _, device in peers:
            send(leaves.at[place], arrives.at[mine], sends, receives, slot, device).wait_send()

    def build_tables():
        inputs[4].wait()
        build_toeplitz(mirrored, toeplitz)
        build_inverse(factors.at[0], factors.at[1], factors.at[2], factors.at[3], table)

    exchange(owners, owner, groups, arrived_groups, group_send, group_recv, build_tables)
    pack_beams(arrived_groups, work, beams)
    exchange(frames, tm, beams, arrived_beams, beam_send, beam_recv)
    gather_frames(arrived_beams, work, gathered)
    invert(gathered, table, series)
    spread(series, blocks)
    correlate(blocks, toeplitz, total)
    pack_echoes(total, work, leaving)
    exchange(frames, tm, leaving, returned, out_send, out_recv)
    unpack_echoes(returned, work)

    done = pltpu.make_async_copy(work, out_hbm, local_sem.at[5])
    done.start()
    for half in range(2):
        for ahead in RING8[:-1]:
            bin_copy(half, ahead, hyd).wait_send()
    drain(owners, owner, groups, arrived_groups, group_send, group_recv)
    drain(frames, tm, beams, arrived_beams, beam_send, beam_recv)
    drain(frames, tm, leaving, returned, out_send, out_recv)
    done.wait()


def ping(spectra, row_lags, col_lags, replica, rep_len):
    factors = jnp.asarray(np.stack(inverse_factors()))
    smem = pl.BlockSpec(memory_space=pltpu.SMEM)
    hbm = pl.BlockSpec(memory_space=pl.ANY)
    bf16, f32, i32 = jnp.bfloat16, jnp.float32, jnp.int32
    dma = pltpu.SemaphoreType.DMA
    return pl.pallas_call(
        ping_kernel,
        out_shape=jax.ShapeDtypeStruct((256, 128), f32),
        in_specs=[smem, smem] + [hbm] * 5,
        out_specs=hbm,
        scratch_shapes=[
            pltpu.VMEM((2, 256, 256), bf16),
            pltpu.VMEM((COLS, BEAMS), i32),
            pltpu.VMEM((ROWS, BEAMS), i32),
            pltpu.VMEM((2, REPLICA), bf16),
            pltpu.VMEM((4, 32, BINS), f32),
            pltpu.VMEM((8, 2, LOCAL_BINS, 256), bf16),
            pltpu.VMEM((COLS, 2 * BEAMS), f32),
            pltpu.VMEM((COLS, 2 * BEAMS), f32),
            pltpu.VMEM((ROWS, 2 * BEAMS), f32),
            pltpu.VMEM((ROWS, 2 * BEAMS), f32),
            pltpu.VMEM((LOCAL_BINS, 128, 2 * BEAMS), bf16),
            pltpu.VMEM((LOCAL_BINS, ROWS, 2 * BEAMS), f32),
            pltpu.VMEM((1024, 128), f32),
            pltpu.VMEM((128, BEAMS), f32),
            pltpu.VMEM((32, 8, 128), bf16),
            pltpu.VMEM((32, 8, 128), bf16),
            pltpu.VMEM((256, 128), f32),
            pltpu.VMEM((16, 16, 128), bf16),
            pltpu.VMEM((16, 16, 128), bf16),
            pltpu.VMEM((16, 2048), bf16),
            pltpu.VMEM((144, 128), f32),
            pltpu.VMEM((144, 128), f32),
            pltpu.VMEM((TAPS * 128, 256), bf16),
            pltpu.VMEM((2048, 2048), bf16),
            pltpu.VMEM((2, 8, 24, 128), f32),
            pltpu.VMEM((2, 72 * 16, 128), bf16),
            pltpu.VMEM((256, 256), f32),
            pltpu.VMEM((16, 16, 128), bf16),
            pltpu.VMEM((16, 16, 128), bf16),
            dma((6,)),
            dma((16,)),
            dma((16,)),
            dma((32,)),
            dma((32,)),
            dma((16,)),
            dma((16,)),
            dma((16,)),
            dma((16,)),
            pltpu.SemaphoreType.REGULAR,
        ],
        compiler_params=pltpu.CompilerParams(
            collective_id=0, has_side_effects=True, vmem_limit_bytes=60 * 1024 * 1024
        ),
    )(jnp.asarray(start_powers()), rep_len, spectra, col_lags, row_lags, replica, factors)


def on_device(spectra, row_lags, col_lags, replica, rep_len):
    returned = ping(spectra, row_lags, col_lags, replica, rep_len)
    return jnp.transpose(returned.reshape(16, 8, 2, 128), (0, 2, 1, 3)).reshape(16, 2, BINS)


def solution(mesh):
    placed = (P(None, "tm", "freq", "hyd"), P(), P(), P(), P())
    return jax.shard_map(
        on_device,
        mesh=mesh,
        in_specs=placed,
        out_specs=P(("hyd", "freq"), None, "tm"),
        check_vma=False,
    )
```

```python
import functools
import math

import jax
import jax.numpy as jnp
import numpy as np
from jax import lax
from jax.experimental import pallas as pl
from jax.experimental.pallas import tpu as pltpu
from jax.sharding import PartitionSpec as P

ROWS = 32
COLS = 64
BINS = 1024
BEAMS = 512
FRAMES = 16
REPLICA = 8192
PERIOD = 2 * BINS
LOCAL_BINS = 32
HALF = LOCAL_BINS // 2
TAPS = REPLICA // 128 + 1


def start_powers():
    table = np.zeros((32, 16), np.float64)
    for place in range(32):
        first = BINS // 2 + place * LOCAL_BINS
        for bit in range(5):
            angle = 2.0 * math.pi * ((first << bit) % PERIOD) / PERIOD
            table[place, 2 * bit] = math.cos(angle)
            table[place, 2 * bit + 1] = math.sin(angle)
    return table.reshape(-1).astype(np.float32)


def inverse_factors():
    n = np.arange(BINS)
    fine = np.exp(2j * np.pi * ((np.arange(32)[:, None] * n) % BINS) / BINS) / math.sqrt(BINS)
    source = np.arange(32)
    first = (source % 4) * 256 + (source // 4) * 32
    coarse = np.exp(2j * np.pi * ((first[:, None] * n) % BINS) / BINS)
    return tuple(part.astype(np.float32) for part in (fine.real, fine.imag, coarse.real, coarse.imag))


def steer(lags, powers, factor):
    re, im = None, None
    for bit in range(5):
        pr, pi = powers[bit]
        chosen = (lags & (1 << bit)) != 0
        if re is None:
            re = jnp.where(chosen, pr * factor, jnp.full(lags.shape, factor, jnp.float32))
            im = jnp.where(chosen, pi * factor, jnp.zeros(lags.shape, jnp.float32))
        else:
            moved_re = re * pr - im * pi
            moved_im = re * pi + im * pr
            re = jnp.where(chosen, moved_re, re)
            im = jnp.where(chosen, moved_im, im)
    return re, im


def begin_steering(place, powers_ref, col_lags_ref, row_lags_ref, col, col_step, row, row_step):
    first = [
        (powers_ref[place * 16 + 2 * bit], powers_ref[place * 16 + 2 * bit + 1]) for bit in range(5)
    ]
    step = [
        (
            np.float32(math.cos(2.0 * math.pi * (1 << bit) / PERIOD)),
            np.float32(math.sin(2.0 * math.pi * (1 << bit) / PERIOD)),
        )
        for bit in range(5)
    ]
    for lags_ref, state, change, count, factor in (
        (col_lags_ref, col, col_step, COLS, COLS**-0.5),
        (row_lags_ref, row, row_step, ROWS, ROWS**-0.5),
    ):

        @pl.loop(0, count // 8)
        def _(group):
            rows = pl.ds(pl.multiple_of(group * 8, 8), 8)
            lags = lags_ref[rows, :]
            re, im = steer(lags, first, np.float32(factor))
            state[rows, 0:BEAMS] = re
            state[rows, BEAMS : 2 * BEAMS] = im
            re, im = steer(lags, step, np.float32(1.0))
            change[rows, 0:BEAMS] = re
            change[rows, BEAMS : 2 * BEAMS] = im


def advance(state, change, rows):
    re = state[rows, 0:BEAMS]
    im = state[rows, BEAMS : 2 * BEAMS]
    cr = change[rows, 0:BEAMS]
    ci = change[rows, BEAMS : 2 * BEAMS]
    state[rows, 0:BEAMS] = re * cr - im * ci
    state[rows, BEAMS : 2 * BEAMS] = re * ci + im * cr
    return re, im


def arrange_sensors(arrived, sensors, half):
    low = lax.broadcasted_iota(jnp.int32, (HALF, 128), 1) < 64
    bins = pl.ds(pl.multiple_of(half * HALF, HALF), HALF)
    for source in range(8):
        for pair in range(2):
            cols = slice(128 * pair, 128 * pair + 128)
            re = arrived[source, 0, bins, cols].astype(jnp.float32)
            im = arrived[source, 1, bins, cols].astype(jnp.float32)
            row = source * 4 + pair * 2
            start = pl.multiple_of(half * HALF, HALF)
            sensors[pl.ds(row * 32 + start, HALF), :] = jnp.where(low, re, pltpu.roll(im, 64, 1))
            sensors[pl.ds(row * 32 + 32 + start, HALF), :] = jnp.where(low, pltpu.roll(re, 64, 1), im)


def build_steering(col, col_step, row, row_step, weights, row_table):
    @pl.loop(0, LOCAL_BINS)
    def _(bin_at):
        for group in range(COLS // 16):
            rows = slice(16 * group, 16 * group + 16)
            re, im = advance(col, col_step, rows)
            weights[bin_at, rows, 0:BEAMS] = re.astype(jnp.bfloat16)
            weights[bin_at, rows, BEAMS : 2 * BEAMS] = im.astype(jnp.bfloat16)
            rows = slice(64 + 16 * group, 64 + 16 * group + 16)
            weights[bin_at, rows, 0:BEAMS] = (-im).astype(jnp.bfloat16)
            weights[bin_at, rows, BEAMS : 2 * BEAMS] = re.astype(jnp.bfloat16)
        for group in range(ROWS // 8):
            rows = slice(8 * group, 8 * group + 8)
            re, im = advance(row, row_step, rows)
            row_table[bin_at, rows, 0:BEAMS] = re
            row_table[bin_at, rows, BEAMS : 2 * BEAMS] = im


def form_beams(sensors, weights, row_table, formed, half):
    @pl.loop(0, HALF, unroll=4)
    def _(step):
        bin_at = half * HALF + step
        data = sensors[pl.ds(bin_at, 32, stride=32), :].astype(jnp.bfloat16)
        along = jnp.dot(data, weights[bin_at], preferred_element_type=jnp.float32)
        row_re = row_table[bin_at, :, 0:BEAMS]
        row_im = row_table[bin_at, :, BEAMS : 2 * BEAMS]
        along_re = along[:, 0:BEAMS]
        along_im = along[:, BEAMS:]
        formed[pl.ds(bin_at, 1), :] = jnp.sum(along_re * row_re - along_im * row_im, axis=0, keepdims=True)
        formed[pl.ds(32 + bin_at, 1), :] = jnp.sum(along_re * row_im + along_im * row_re, axis=0, keepdims=True)


def pack_groups(formed, groups):
    low = lax.broadcasted_iota(jnp.int32, (8, 128), 1) < 64

    @pl.loop(0, 4)
    def _(quarter):
        turned = formed[:, pl.ds(pl.multiple_of(128 * quarter, 128), 128)].T
        for member in range(8):
            first = turned[16 * member : 16 * member + 8]
            second = turned[16 * member + 8 : 16 * member + 16]
            packed = jnp.where(low, first, pltpu.roll(second, 64, 1))
            groups[8 * quarter + member] = packed.astype(jnp.bfloat16)


def pack_beams(arrived, work, beams):
    low = lax.broadcasted_iota(jnp.int32, (8, 128), 1) < 64
    for pair in range(16):
        first = arrived[2 * pair].astype(jnp.float32)
        second = arrived[2 * pair + 1].astype(jnp.float32)
        work[8 * pair : 8 * pair + 8, :] = jnp.where(low, first, pltpu.roll(second, 64, 1))
        work[128 + 8 * pair : 136 + 8 * pair, :] = jnp.where(low, pltpu.roll(first, 64, 1), second)
    for beam in range(16):
        start = 128 * (beam // 8) + beam % 8
        beams[beam] = work[pl.ds(start, 16, stride=8), :].astype(jnp.bfloat16)


def gather_frames(arrived, work, gathered):
    for frame in range(FRAMES):
        work[16 * frame : 16 * frame + 16, :] = arrived[frame].astype(jnp.float32)
    for pair in range(16):
        gathered[:, 128 * pair : 128 * pair + 128] = work[pl.ds(pair, 16, stride=16), :].astype(jnp.bfloat16)


def lay_pulse(replica, length, lines, mirrored):
    lines[...] = jnp.zeros_like(lines)
    lane = lax.broadcasted_iota(jnp.int32, (2, 128), 1)
    for tap in range(TAPS - 1):
        line = replica[:, 128 * tap : 128 * tap + 128].astype(jnp.float32)
        lines[2 + 2 * tap : 4 + 2 * tap, :] = jnp.where(lane + 128 * tap < length, line, 0.0)
    down = lax.broadcasted_iota(jnp.int32, (128, 128), 0)
    across = lax.broadcasted_iota(jnp.int32, (128, 128), 1)
    turn = jnp.where((down + across) % 128 == 0, 1.0, 0.0).astype(jnp.bfloat16)
    mirrored[...] = jnp.dot(lines[...].astype(jnp.bfloat16), turn, preferred_element_type=jnp.float32)


def build_toeplitz(mirrored, toeplitz):
    down = lax.broadcasted_iota(jnp.int32, (128, 128), 0)
    across = lax.broadcasted_iota(jnp.int32, (128, 128), 1)
    lower = down >= across

    @pl.loop(0, TAPS // 5)
    def _(group):
        for part in range(2):
            turned = []
            for member in range(6):
                line = mirrored[pl.ds(2 * (group * 5 + member) + part, 1), :]
                turned.append(pltpu.roll(jnp.broadcast_to(line, (128, 128)), 0, 1, stride=1, stride_axis=0))
            for member in range(5):
                rows = pl.ds(pl.multiple_of((group * 5 + member) * 128, 128), 128)
                both = jnp.where(lower, turned[member + 1], turned[member])
                toeplitz[rows, 128 * part : 128 * part + 128] = both.astype(jnp.bfloat16)


def build_inverse(fine_re_ref, fine_im_ref, coarse_re_ref, coarse_im_ref, table):
    @pl.loop(0, 32)
    def _(source):
        start = pl.multiple_of(source * 64, 64)
        for half in range(2):
            for block in range(4):
                cols = slice(256 * block, 256 * block + 256)
                fr = fine_re_ref[16 * half : 16 * half + 16, cols]
                fi = fine_im_ref[16 * half : 16 * half + 16, cols]
                cr = coarse_re_ref[pl.ds(source, 1), cols]
                ci = coarse_im_ref[pl.ds(source, 1), cols]
                re = fr * cr - fi * ci
                im = fr * ci + fi * cr
                rows = pl.ds(start + 16 * half, 16)
                table[rows, cols] = re.astype(jnp.bfloat16)
                table[rows, slice(1024 + 256 * block, 1280 + 256 * block)] = im.astype(jnp.bfloat16)
                rows = pl.ds(start + 32 + 16 * half, 16)
                table[rows, cols] = (-im).astype(jnp.bfloat16)
                table[rows, slice(1024 + 256 * block, 1280 + 256 * block)] = re.astype(jnp.bfloat16)


def invert(gathered, table, series):
    series[...] = jnp.zeros_like(series)

    @pl.loop(0, 4)
    def _(block):
        cols = pl.ds(pl.multiple_of(512 * block, 512), 512)
        total = jnp.dot(gathered[...], table[:, cols], preferred_element_type=jnp.float32)
        for side in range(4):
            series[block // 2, 4 * (block % 2) + side, 0:16, :] = total[:, 128 * side : 128 * side + 128]


def spread(series, blocks):
    for part in range(2):
        for index in range(72):
            ahead, block = index // 8, index % 8
            blocks[part, 16 * index : 16 * index + 16, :] = series[part, block, ahead : ahead + 16, :].astype(
                jnp.bfloat16
            )


def correlate(blocks, toeplitz, total):
    def lines(tap):
        return jnp.concatenate(
            [blocks[part, pl.ds(pl.multiple_of(tap * 16, 16), 128), :] for part in range(2)], axis=0
        )

    last = TAPS - 1
    total[...] = jnp.dot(lines(last), toeplitz[128 * last : 128 * TAPS, :], preferred_element_type=jnp.float32)

    @pl.loop(0, last // 16)
    def _(group):
        tap = group * 16
        data = jnp.concatenate([lines(tap + member) for member in range(16)], axis=1)
        weights = toeplitz[pl.ds(pl.multiple_of(tap * 128, 16 * 128), 16 * 128), :]
        total[...] += jnp.dot(data, weights, preferred_element_type=jnp.float32)


def pack_echoes(total, work, leaving):
    for block in range(8):
        rows = slice(16 * block, 16 * block + 16)
        after = slice(128 + 16 * block, 144 + 16 * block)
        work[pl.ds(2 * block, 16, stride=16), :] = total[rows, 0:128] + total[after, 128:256]
        work[pl.ds(2 * block + 1, 16, stride=16), :] = total[after, 0:128] - total[rows, 128:256]
    for frame in range(FRAMES):
        leaving[frame] = work[16 * frame : 16 * frame + 16, :].astype(jnp.bfloat16)


def unpack_echoes(returned, work):
    for beam in range(16):
        work[16 * beam : 16 * beam + 16, :] = returned[beam].astype(jnp.float32)


RING8 = (4, 3, 5, 2, 6, 1, 7, 0)
RING4 = (2, 1, 3, 0)


def send(source, target, sends, receives, slot, device):
    return pltpu.make_async_remote_copy(
        src_ref=source,
        dst_ref=target,
        send_sem=sends.at[slot],
        recv_sem=receives.at[slot],
        device_id=device,
        device_id_type=pl.DeviceIdType.MESH,
    )


def ping_kernel(
    powers_ref,
    length_ref,
    spectra_hbm,
    col_lags_hbm,
    row_lags_hbm,
    replica_hbm,
    factors_hbm,
    out_ref,
    spectra,
    col_lags,
    row_lags,
    replica,
    factors,
    arrived_bins,
    col,
    col_step,
    row,
    row_step,
    weights,
    row_table,
    sensors,
    formed,
    groups,
    arrived_groups,
    work,
    beams,
    arrived_beams,
    gathered,
    lines,
    mirrored,
    toeplitz,
    table,
    series,
    blocks,
    total,
    leaving,
    returned,
    local_sem,
    bin_send,
    bin_recv,
    group_send,
    group_recv,
    beam_send,
    beam_recv,
    out_send,
    out_recv,
    relayed,
):
    hyd = lax.axis_index("hyd")
    freq = lax.axis_index("freq")
    tm = lax.axis_index("tm")
    owner = hyd * 4 + freq

    inputs = [
        pltpu.make_async_copy(source, target, local_sem.at[index])
        for index, (source, target) in enumerate(
            (
                (spectra_hbm.at[:, 0], spectra),
                (col_lags_hbm, col_lags),
                (row_lags_hbm, row_lags),
                (replica_hbm, replica),
                (factors_hbm, factors),
            )
        )
    ]
    inputs[0].start()

    owners = []
    for ahead in RING8:
        for side in range(4):
            if ahead or side:
                to = ((hyd + ahead) & 7, (freq + side) & 3)
                back = ((hyd - ahead) & 7, (freq - side) & 3)
                owners.append((ahead * 4 + side, to[0] * 4 + to[1], back[0] * 4 + back[1], {"hyd": to[0], "freq": to[1]}))
    frames = []
    for far in RING4:
        for near in RING4:
            if far or near:
                to = ((((tm >> 2) + far) & 3) * 4) + ((tm + near) & 3)
                back = ((((tm >> 2) - far) & 3) * 4) + ((tm - near) & 3)
                frames.append((far * 4 + near, to, back, {"tm": to}))

    barrier = pltpu.get_barrier_semaphore()
    beside = [{"freq": (freq + side) & 3} for side in range(1, 4)]
    near = [{"tm": (tm & 12) + ((tm + step) & 3)} for step in range(1, 4)]
    along = [{"hyd": (hyd + ahead) & 7} for ahead in RING8[:-1]]
    across = [{"tm": (tm + 4 * step) & 15} for step in range(1, 4)]
    for device in along + across + near + beside:
        pl.semaphore_signal(barrier, inc=1, device_id=device, device_id_type=pl.DeviceIdType.MESH)

    for copy in inputs[1:]:
        copy.start()
    inputs[0].wait()
    pl.semaphore_wait(barrier, 16)

    def bin_copy(half, ahead, source):
        place = (hyd + ahead) & 7
        start = pl.multiple_of(place * LOCAL_BINS + half * HALF, HALF)
        bins = pl.ds(pl.multiple_of(half * HALF, HALF), HALF)
        return send(
            spectra.at[:, pl.ds(start, HALF), :],
            arrived_bins.at[source, :, bins, :],
            bin_send,
            bin_recv,
            half * 8 + ahead,
            {"hyd": place},
        )

    for half in range(2):
        for ahead in RING8[:-1]:
            bin_copy(half, ahead, hyd).start()
    mine = pl.ds(pl.multiple_of(hyd * LOCAL_BINS, LOCAL_BINS), LOCAL_BINS)
    own = pltpu.make_async_copy(spectra.at[:, mine, :], arrived_bins.at[hyd], local_sem.at[5])
    own.start()
    for device in near + beside:
        pl.semaphore_signal(relayed, inc=1, device_id=device, device_id_type=pl.DeviceIdType.MESH)

    inputs[1].wait()
    inputs[2].wait()
    begin_steering(freq * 8 + hyd, powers_ref, col_lags, row_lags, col, col_step, row, row_step)
    build_steering(col, col_step, row, row_step, weights, row_table)
    inputs[3].wait()
    lay_pulse(replica, length_ref[0], lines, mirrored)
    formed[64:128, :] = jnp.zeros((64, BEAMS), jnp.float32)
    own.wait()

    @pl.loop(0, 2)
    def _(half):
        for ahead in RING8[-2::-1]:
            bin_copy(half, ahead, (hyd - ahead) & 7).wait_recv()
        arrange_sensors(arrived_bins, sensors, half)
        form_beams(sensors, weights, row_table, formed, half)

    pack_groups(formed, groups)
    pl.semaphore_wait(relayed, 6)

    def exchange(peers, mine, leaves, arrives, sends, receives, meanwhile=None):
        def copy(slot, place, source, device):
            return send(leaves.at[place], arrives.at[source], sends, receives, slot, device)

        for slot, place, _, device in peers:
            copy(slot, place, mine, device).start()
        own = pltpu.make_async_copy(leaves.at[mine], arrives.at[mine], local_sem.at[5])
        own.start()
        if meanwhile is not None:
            meanwhile()
        own.wait()
        for slot, place, source, device in peers[::-1]:
            copy(slot, place, source, device).wait_recv()

    def drain(peers, mine, leaves, arrives, sends, receives):
        for slot, place, _, device in peers:
            send(leaves.at[place], arrives.at[mine], sends, receives, slot, device).wait_send()

    def build_tables():
        inputs[4].wait()
        build_toeplitz(mirrored, toeplitz)
        build_inverse(factors.at[0], factors.at[1], factors.at[2], factors.at[3], table)

    exchange(owners, owner, groups, arrived_groups, group_send, group_recv, build_tables)
    pack_beams(arrived_groups, work, beams)
    exchange(frames, tm, beams, arrived_beams, beam_send, beam_recv)
    gather_frames(arrived_beams, work, gathered)
    invert(gathered, table, series)
    spread(series, blocks)
    correlate(blocks, toeplitz, total)
    pack_echoes(total, work, leaving)
    exchange(frames, tm, leaving, returned, out_send, out_recv)
    unpack_echoes(returned, out_ref)

    for half in range(2):
        for ahead in RING8[:-1]:
            bin_copy(half, ahead, hyd).wait_send()
    drain(owners, owner, groups, arrived_groups, group_send, group_recv)
    drain(frames, tm, beams, arrived_beams, beam_send, beam_recv)
    drain(frames, tm, leaving, returned, out_send, out_recv)


def ping(spectra, row_lags, col_lags, replica, rep_len):
    factors = jnp.asarray(np.stack(inverse_factors()))
    smem = pl.BlockSpec(memory_space=pltpu.SMEM)
    hbm = pl.BlockSpec(memory_space=pl.ANY)
    bf16, f32, i32 = jnp.bfloat16, jnp.float32, jnp.int32
    dma = pltpu.SemaphoreType.DMA
    return pl.pallas_call(
        ping_kernel,
        out_shape=pltpu.VMEM((256, 128), f32),
        in_specs=[smem, smem] + [hbm] * 5,
        out_specs=pl.BlockSpec(memory_space=pltpu.VMEM),
        scratch_shapes=[
            pltpu.VMEM((2, 256, 256), bf16),
            pltpu.VMEM((COLS, BEAMS), i32),
            pltpu.VMEM((ROWS, BEAMS), i32),
            pltpu.VMEM((2, REPLICA), bf16),
            pltpu.VMEM((4, 32, BINS), f32),
            pltpu.VMEM((8, 2, LOCAL_BINS, 256), bf16),
            pltpu.VMEM((COLS, 2 * BEAMS), f32),
            pltpu.VMEM((COLS, 2 * BEAMS), f32),
            pltpu.VMEM((ROWS, 2 * BEAMS), f32),
            pltpu.VMEM((ROWS, 2 * BEAMS), f32),
            pltpu.VMEM((LOCAL_BINS, 128, 2 * BEAMS), bf16),
            pltpu.VMEM((LOCAL_BINS, ROWS, 2 * BEAMS), f32),
            pltpu.VMEM((1024, 128), f32),
            pltpu.VMEM((128, BEAMS), f32),
            pltpu.VMEM((32, 8, 128), bf16),
            pltpu.VMEM((32, 8, 128), bf16),
            pltpu.VMEM((256, 128), f32),
            pltpu.VMEM((16, 16, 128), bf16),
            pltpu.VMEM((16, 16, 128), bf16),
            pltpu.VMEM((16, 2048), bf16),
            pltpu.VMEM((144, 128), f32),
            pltpu.VMEM((144, 128), f32),
            pltpu.VMEM((TAPS * 128, 256), bf16),
            pltpu.VMEM((2048, 2048), bf16),
            pltpu.VMEM((2, 8, 24, 128), f32),
            pltpu.VMEM((2, 72 * 16, 128), bf16),
            pltpu.VMEM((256, 256), f32),
            pltpu.VMEM((16, 16, 128), bf16),
            pltpu.VMEM((16, 16, 128), bf16),
            dma((6,)),
            dma((16,)),
            dma((16,)),
            dma((32,)),
            dma((32,)),
            dma((16,)),
            dma((16,)),
            dma((16,)),
            dma((16,)),
            pltpu.SemaphoreType.REGULAR,
        ],
        compiler_params=pltpu.CompilerParams(
            collective_id=0, has_side_effects=True, vmem_limit_bytes=60 * 1024 * 1024
        ),
    )(jnp.asarray(start_powers()), rep_len, spectra, col_lags, row_lags, replica, factors)


def on_device(spectra, row_lags, col_lags, replica, rep_len):
    returned = ping(spectra, row_lags, col_lags, replica, rep_len)
    return jnp.transpose(returned.reshape(16, 8, 2, 128), (0, 2, 1, 3)).reshape(16, 2, BINS)


def solution(mesh):
    placed = (P(None, "tm", "freq", "hyd"), P(), P(), P(), P())
    return jax.shard_map(
        on_device,
        mesh=mesh,
        in_specs=placed,
        out_specs=P(("hyd", "freq"), None, "tm"),
        check_vma=False,
    )
```

```python
import functools
import math

import jax
import jax.numpy as jnp
import numpy as np
from jax import lax
from jax.experimental import pallas as pl
from jax.experimental.pallas import tpu as pltpu
from jax.sharding import PartitionSpec as P

ROWS = 32
COLS = 64
BINS = 1024
BEAMS = 512
FRAMES = 16
REPLICA = 8192
PERIOD = 2 * BINS
LOCAL_BINS = 32
HALF = LOCAL_BINS // 2
TAPS = REPLICA // 128 + 1


def start_powers():
    table = np.zeros((32, 16), np.float64)
    for place in range(32):
        first = BINS // 2 + place * LOCAL_BINS
        for bit in range(5):
            angle = 2.0 * math.pi * ((first << bit) % PERIOD) / PERIOD
            table[place, 2 * bit] = math.cos(angle)
            table[place, 2 * bit + 1] = math.sin(angle)
    return table.reshape(-1).astype(np.float32)


def inverse_factors():
    n = np.arange(BINS)
    fine = np.exp(2j * np.pi * ((np.arange(32)[:, None] * n) % BINS) / BINS) / math.sqrt(BINS)
    source = np.arange(32)
    first = (source % 4) * 256 + (source // 4) * 32
    coarse = np.exp(2j * np.pi * ((first[:, None] * n) % BINS) / BINS)
    return tuple(part.astype(np.float32) for part in (fine.real, fine.imag, coarse.real, coarse.imag))


def steer(lags, powers, factor):
    re, im = None, None
    for bit in range(5):
        pr, pi = powers[bit]
        chosen = (lags & (1 << bit)) != 0
        if re is None:
            re = jnp.where(chosen, pr * factor, jnp.full(lags.shape, factor, jnp.float32))
            im = jnp.where(chosen, pi * factor, jnp.zeros(lags.shape, jnp.float32))
        else:
            moved_re = re * pr - im * pi
            moved_im = re * pi + im * pr
            re = jnp.where(chosen, moved_re, re)
            im = jnp.where(chosen, moved_im, im)
    return re, im


def begin_steering(place, powers_ref, col_lags_ref, row_lags_ref, col, col_step, row, row_step):
    first = [
        (powers_ref[place * 16 + 2 * bit], powers_ref[place * 16 + 2 * bit + 1]) for bit in range(5)
    ]
    step = [
        (
            np.float32(math.cos(2.0 * math.pi * (1 << bit) / PERIOD)),
            np.float32(math.sin(2.0 * math.pi * (1 << bit) / PERIOD)),
        )
        for bit in range(5)
    ]
    for lags_ref, state, change, count, factor in (
        (col_lags_ref, col, col_step, COLS, COLS**-0.5),
        (row_lags_ref, row, row_step, ROWS, ROWS**-0.5),
    ):

        @pl.loop(0, count // 8)
        def _(group):
            rows = pl.ds(pl.multiple_of(group * 8, 8), 8)
            lags = lags_ref[rows, :]
            re, im = steer(lags, first, np.float32(factor))
            state[rows, 0:BEAMS] = re
            state[rows, BEAMS : 2 * BEAMS] = im
            re, im = steer(lags, step, np.float32(1.0))
            change[rows, 0:BEAMS] = re
            change[rows, BEAMS : 2 * BEAMS] = im


def advance(state, change, rows):
    re = state[rows, 0:BEAMS]
    im = state[rows, BEAMS : 2 * BEAMS]
    cr = change[rows, 0:BEAMS]
    ci = change[rows, BEAMS : 2 * BEAMS]
    state[rows, 0:BEAMS] = re * cr - im * ci
    state[rows, BEAMS : 2 * BEAMS] = re * ci + im * cr
    return re, im


def arrange_sensors(arrived, sensors, half):
    low = lax.broadcasted_iota(jnp.int32, (HALF, 128), 1) < 64
    bins = pl.ds(pl.multiple_of(half * HALF, HALF), HALF)
    for source in range(8):
        for pair in range(2):
            cols = slice(128 * pair, 128 * pair + 128)
            re = arrived[source, 0, bins, cols].astype(jnp.float32)
            im = arrived[source, 1, bins, cols].astype(jnp.float32)
            row = source * 4 + pair * 2
            start = pl.multiple_of(half * HALF, HALF)
            sensors[pl.ds(row * 32 + start, HALF), :] = jnp.where(low, re, pltpu.roll(im, 64, 1))
            sensors[pl.ds(row * 32 + 32 + start, HALF), :] = jnp.where(low, pltpu.roll(re, 64, 1), im)


def build_steering(col, col_step, row, row_step, weights, row_table):
    @pl.loop(0, LOCAL_BINS)
    def _(bin_at):
        for group in range(COLS // 16):
            rows = slice(16 * group, 16 * group + 16)
            re, im = advance(col, col_step, rows)
            weights[bin_at, rows, 0:BEAMS] = re.astype(jnp.bfloat16)
            weights[bin_at, rows, BEAMS : 2 * BEAMS] = im.astype(jnp.bfloat16)
            rows = slice(64 + 16 * group, 64 + 16 * group + 16)
            weights[bin_at, rows, 0:BEAMS] = (-im).astype(jnp.bfloat16)
            weights[bin_at, rows, BEAMS : 2 * BEAMS] = re.astype(jnp.bfloat16)
        for group in range(ROWS // 8):
            rows = slice(8 * group, 8 * group + 8)
            re, im = advance(row, row_step, rows)
            row_table[bin_at, rows, 0:BEAMS] = re
            row_table[bin_at, rows, BEAMS : 2 * BEAMS] = im


def form_beams(sensors, weights, row_table, formed, half):
    @pl.loop(0, HALF, unroll=8)
    def _(step):
        bin_at = half * HALF + step
        data = sensors[pl.ds(bin_at, 32, stride=32), :].astype(jnp.bfloat16)
        along = jnp.dot(data, weights[bin_at], preferred_element_type=jnp.float32)
        row_re = row_table[bin_at, :, 0:BEAMS]
        row_im = row_table[bin_at, :, BEAMS : 2 * BEAMS]
        along_re = along[:, 0:BEAMS]
        along_im = along[:, BEAMS:]
        formed[pl.ds(bin_at, 1), :] = jnp.sum(along_re * row_re - along_im * row_im, axis=0, keepdims=True)
        formed[pl.ds(32 + bin_at, 1), :] = jnp.sum(along_re * row_im + along_im * row_re, axis=0, keepdims=True)


def pack_groups(formed, groups):
    low = lax.broadcasted_iota(jnp.int32, (8, 128), 1) < 64

    @pl.loop(0, 4, unroll=2)
    def _(quarter):
        turned = formed[:, pl.ds(pl.multiple_of(128 * quarter, 128), 128)].T
        for member in range(8):
            first = turned[16 * member : 16 * member + 8]
            second = turned[16 * member + 8 : 16 * member + 16]
            packed = jnp.where(low, first, pltpu.roll(second, 64, 1))
            groups[8 * quarter + member] = packed.astype(jnp.bfloat16)


def pack_beams(arrived, work, beams):
    low = lax.broadcasted_iota(jnp.int32, (8, 128), 1) < 64
    for pair in range(16):
        first = arrived[2 * pair].astype(jnp.float32)
        second = arrived[2 * pair + 1].astype(jnp.float32)
        work[8 * pair : 8 * pair + 8, :] = jnp.where(low, first, pltpu.roll(second, 64, 1))
        work[128 + 8 * pair : 136 + 8 * pair, :] = jnp.where(low, pltpu.roll(first, 64, 1), second)
    for beam in range(16):
        start = 128 * (beam // 8) + beam % 8
        beams[beam] = work[pl.ds(start, 16, stride=8), :].astype(jnp.bfloat16)


def gather_frames(arrived, work, gathered):
    for frame in range(FRAMES):
        work[16 * frame : 16 * frame + 16, :] = arrived[frame].astype(jnp.float32)
    for pair in range(16):
        gathered[:, 128 * pair : 128 * pair + 128] = work[pl.ds(pair, 16, stride=16), :].astype(jnp.bfloat16)


def lay_pulse(replica, length, lines, mirrored):
    lines[...] = jnp.zeros_like(lines)
    lane = lax.broadcasted_iota(jnp.int32, (2, 128), 1)
    for tap in range(TAPS - 1):
        line = replica[:, 128 * tap : 128 * tap + 128].astype(jnp.float32)
        lines[2 + 2 * tap : 4 + 2 * tap, :] = jnp.where(lane + 128 * tap < length, line, 0.0)
    down = lax.broadcasted_iota(jnp.int32, (128, 128), 0)
    across = lax.broadcasted_iota(jnp.int32, (128, 128), 1)
    turn = jnp.where((down + across) % 128 == 0, 1.0, 0.0).astype(jnp.bfloat16)
    mirrored[...] = jnp.dot(lines[...].astype(jnp.bfloat16), turn, preferred_element_type=jnp.float32)


def build_toeplitz(mirrored, toeplitz):
    down = lax.broadcasted_iota(jnp.int32, (128, 128), 0)
    across = lax.broadcasted_iota(jnp.int32, (128, 128), 1)
    lower = down >= across

    @pl.loop(0, TAPS // 5)
    def _(group):
        for part in range(2):
            turned = []
            for member in range(6):
                line = mirrored[pl.ds(2 * (group * 5 + member) + part, 1), :]
                turned.append(pltpu.roll(jnp.broadcast_to(line, (128, 128)), 0, 1, stride=1, stride_axis=0))
            for member in range(5):
                rows = pl.ds(pl.multiple_of((group * 5 + member) * 128, 128), 128)
                both = jnp.where(lower, turned[member + 1], turned[member])
                toeplitz[rows, 128 * part : 128 * part + 128] = both.astype(jnp.bfloat16)


def build_inverse(fine_re_ref, fine_im_ref, coarse_re_ref, coarse_im_ref, table):
    @pl.loop(0, 32)
    def _(source):
        start = pl.multiple_of(source * 64, 64)
        for half in range(2):
            for block in range(4):
                cols = slice(256 * block, 256 * block + 256)
                fr = fine_re_ref[16 * half : 16 * half + 16, cols]
                fi = fine_im_ref[16 * half : 16 * half + 16, cols]
                cr = coarse_re_ref[pl.ds(source, 1), cols]
                ci = coarse_im_ref[pl.ds(source, 1), cols]
                re = fr * cr - fi * ci
                im = fr * ci + fi * cr
                rows = pl.ds(start + 16 * half, 16)
                table[rows, cols] = re.astype(jnp.bfloat16)
                table[rows, slice(1024 + 256 * block, 1280 + 256 * block)] = im.astype(jnp.bfloat16)
                rows = pl.ds(start + 32 + 16 * half, 16)
                table[rows, cols] = (-im).astype(jnp.bfloat16)
                table[rows, slice(1024 + 256 * block, 1280 + 256 * block)] = re.astype(jnp.bfloat16)


def invert(gathered, table, series):
    series[...] = jnp.zeros_like(series)

    @pl.loop(0, 4, unroll=2)
    def _(block):
        cols = pl.ds(pl.multiple_of(512 * block, 512), 512)
        total = jnp.dot(gathered[...], table[:, cols], preferred_element_type=jnp.float32)
        for side in range(4):
            series[block // 2, 4 * (block % 2) + side, 0:16, :] = total[:, 128 * side : 128 * side + 128]


def spread(series, blocks):
    for part in range(2):
        for index in range(72):
            ahead, block = index // 8, index % 8
            blocks[part, 16 * index : 16 * index + 16, :] = series[part, block, ahead : ahead + 16, :].astype(
                jnp.bfloat16
            )


def correlate(blocks, toeplitz, total):
    def lines(tap):
        return jnp.concatenate(
            [blocks[part, pl.ds(pl.multiple_of(tap * 16, 16), 128), :] for part in range(2)], axis=0
        )

    last = TAPS - 1
    total[...] = jnp.dot(lines(last), toeplitz[128 * last : 128 * TAPS, :], preferred_element_type=jnp.float32)

    @pl.loop(0, last // 32)
    def _(group):
        tap = group * 32
        data = jnp.concatenate([lines(tap + member) for member in range(32)], axis=1)
        weights = toeplitz[pl.ds(pl.multiple_of(tap * 128, 32 * 128), 32 * 128), :]
        total[...] += jnp.dot(data, weights, preferred_element_type=jnp.float32)


def pack_echoes(total, work, leaving):
    for block in range(8):
        rows = slice(16 * block, 16 * block + 16)
        after = slice(128 + 16 * block, 144 + 16 * block)
        work[pl.ds(2 * block, 16, stride=16), :] = total[rows, 0:128] + total[after, 128:256]
        work[pl.ds(2 * block + 1, 16, stride=16), :] = total[after, 0:128] - total[rows, 128:256]
    for frame in range(FRAMES):
        leaving[frame] = work[16 * frame : 16 * frame + 16, :].astype(jnp.bfloat16)


def unpack_echoes(returned, work):
    for beam in range(16):
        work[16 * beam : 16 * beam + 16, :] = returned[beam].astype(jnp.float32)


RING8 = (4, 3, 5, 2, 6, 1, 7, 0)
RING4 = (2, 1, 3, 0)


def send(source, target, sends, receives, slot, device):
    return pltpu.make_async_remote_copy(
        src_ref=source,
        dst_ref=target,
        send_sem=sends.at[slot],
        recv_sem=receives.at[slot],
        device_id=device,
        device_id_type=pl.DeviceIdType.MESH,
    )


def ping_kernel(
    powers_ref,
    length_ref,
    spectra_hbm,
    col_lags_hbm,
    row_lags_hbm,
    replica_hbm,
    factors_hbm,
    out_ref,
    spectra,
    col_lags,
    row_lags,
    replica,
    factors,
    arrived_bins,
    col,
    col_step,
    row,
    row_step,
    weights,
    row_table,
    sensors,
    formed,
    groups,
    arrived_groups,
    work,
    beams,
    arrived_beams,
    gathered,
    lines,
    mirrored,
    toeplitz,
    table,
    series,
    blocks,
    total,
    leaving,
    returned,
    local_sem,
    bin_send,
    bin_recv,
    group_send,
    group_recv,
    beam_send,
    beam_recv,
    out_send,
    out_recv,
    relayed,
):
    hyd = lax.axis_index("hyd")
    freq = lax.axis_index("freq")
    tm = lax.axis_index("tm")
    owner = hyd * 4 + freq

    inputs = [
        pltpu.make_async_copy(source, target, local_sem.at[index])
        for index, (source, target) in enumerate(
            (
                (spectra_hbm.at[:, 0], spectra),
                (col_lags_hbm, col_lags),
                (row_lags_hbm, row_lags),
                (replica_hbm, replica),
                (factors_hbm, factors),
            )
        )
    ]
    inputs[0].start()

    owners = []
    for ahead in RING8:
        for side in range(4):
            if ahead or side:
                to = ((hyd + ahead) & 7, (freq + side) & 3)
                back = ((hyd - ahead) & 7, (freq - side) & 3)
                owners.append((ahead * 4 + side, to[0] * 4 + to[1], back[0] * 4 + back[1], {"hyd": to[0], "freq": to[1]}))
    frames = []
    for far in RING4:
        for near in RING4:
            if far or near:
                to = ((((tm >> 2) + far) & 3) * 4) + ((tm + near) & 3)
                back = ((((tm >> 2) - far) & 3) * 4) + ((tm - near) & 3)
                frames.append((far * 4 + near, to, back, {"tm": to}))

    barrier = pltpu.get_barrier_semaphore()
    beside = [{"freq": (freq + side) & 3} for side in range(1, 4)]
    near = [{"tm": (tm & 12) + ((tm + step) & 3)} for step in range(1, 4)]
    along = [{"hyd": (hyd + ahead) & 7} for ahead in RING8[:-1]]
    across = [{"tm": (tm + 4 * step) & 15} for step in range(1, 4)]
    for device in along + across + near + beside:
        pl.semaphore_signal(barrier, inc=1, device_id=device, device_id_type=pl.DeviceIdType.MESH)

    for copy in inputs[1:]:
        copy.start()
    inputs[0].wait()
    pl.semaphore_wait(barrier, 16)

    def bin_copy(half, ahead, source):
        place = (hyd + ahead) & 7
        start = pl.multiple_of(place * LOCAL_BINS + half * HALF, HALF)
        bins = pl.ds(pl.multiple_of(half * HALF, HALF), HALF)
        return send(
            spectra.at[:, pl.ds(start, HALF), :],
            arrived_bins.at[source, :, bins, :],
            bin_send,
            bin_recv,
            half * 8 + ahead,
            {"hyd": place},
        )

    for half in range(2):
        for ahead in RING8[:-1]:
            bin_copy(half, ahead, hyd).start()
    mine = pl.ds(pl.multiple_of(hyd * LOCAL_BINS, LOCAL_BINS), LOCAL_BINS)
    own = pltpu.make_async_copy(spectra.at[:, mine, :], arrived_bins.at[hyd], local_sem.at[5])
    own.start()
    for device in near + beside:
        pl.semaphore_signal(relayed, inc=1, device_id=device, device_id_type=pl.DeviceIdType.MESH)

    inputs[1].wait()
    inputs[2].wait()
    begin_steering(freq * 8 + hyd, powers_ref, col_lags, row_lags, col, col_step, row, row_step)
    build_steering(col, col_step, row, row_step, weights, row_table)
    inputs[3].wait()
    lay_pulse(replica, length_ref[0], lines, mirrored)
    formed[64:128, :] = jnp.zeros((64, BEAMS), jnp.float32)
    own.wait()

    @pl.loop(0, 2)
    def _(half):
        for ahead in RING8[-2::-1]:
            bin_copy(half, ahead, (hyd - ahead) & 7).wait_recv()
        arrange_sensors(arrived_bins, sensors, half)
        form_beams(sensors, weights, row_table, formed, half)

    pack_groups(formed, groups)
    pl.semaphore_wait(relayed, 6)

    def exchange(peers, mine, leaves, arrives, sends, receives, meanwhile=None):
        def copy(slot, place, source, device):
            return send(leaves.at[place], arrives.at[source], sends, receives, slot, device)

        for slot, place, _, device in peers:
            copy(slot, place, mine, device).start()
        own = pltpu.make_async_copy(leaves.at[mine], arrives.at[mine], local_sem.at[5])
        own.start()
        if meanwhile is not None:
            meanwhile()
        own.wait()
        for slot, place, source, device in peers[::-1]:
            copy(slot, place, source, device).wait_recv()

    def drain(peers, mine, leaves, arrives, sends, receives):
        for slot, place, _, device in peers:
            send(leaves.at[place], arrives.at[mine], sends, receives, slot, device).wait_send()

    def build_tables():
        inputs[4].wait()
        build_toeplitz(mirrored, toeplitz)
        build_inverse(factors.at[0], factors.at[1], factors.at[2], factors.at[3], table)

    exchange(owners, owner, groups, arrived_groups, group_send, group_recv, build_tables)
    pack_beams(arrived_groups, work, beams)
    exchange(frames, tm, beams, arrived_beams, beam_send, beam_recv)
    gather_frames(arrived_beams, work, gathered)
    invert(gathered, table, series)
    spread(series, blocks)
    correlate(blocks, toeplitz, total)
    pack_echoes(total, work, leaving)
    exchange(frames, tm, leaving, returned, out_send, out_recv)
    unpack_echoes(returned, out_ref)

    for half in range(2):
        for ahead in RING8[:-1]:
            bin_copy(half, ahead, hyd).wait_send()
    drain(owners, owner, groups, arrived_groups, group_send, group_recv)
    drain(frames, tm, beams, arrived_beams, beam_send, beam_recv)
    drain(frames, tm, leaving, returned, out_send, out_recv)


def ping(spectra, row_lags, col_lags, replica, rep_len):
    factors = jnp.asarray(np.stack(inverse_factors()))
    smem = pl.BlockSpec(memory_space=pltpu.SMEM)
    hbm = pl.BlockSpec(memory_space=pl.ANY)
    bf16, f32, i32 = jnp.bfloat16, jnp.float32, jnp.int32
    dma = pltpu.SemaphoreType.DMA
    return pl.pallas_call(
        ping_kernel,
        out_shape=pltpu.VMEM((256, 128), f32),
        in_specs=[smem, smem] + [hbm] * 5,
        out_specs=pl.BlockSpec(memory_space=pltpu.VMEM),
        scratch_shapes=[
            pltpu.VMEM((2, 256, 256), bf16),
            pltpu.VMEM((COLS, BEAMS), i32),
            pltpu.VMEM((ROWS, BEAMS), i32),
            pltpu.VMEM((2, REPLICA), bf16),
            pltpu.VMEM((4, 32, BINS), f32),
            pltpu.VMEM((8, 2, LOCAL_BINS, 256), bf16),
            pltpu.VMEM((COLS, 2 * BEAMS), f32),
            pltpu.VMEM((COLS, 2 * BEAMS), f32),
            pltpu.VMEM((ROWS, 2 * BEAMS), f32),
            pltpu.VMEM((ROWS, 2 * BEAMS), f32),
            pltpu.VMEM((LOCAL_BINS, 128, 2 * BEAMS), bf16),
            pltpu.VMEM((LOCAL_BINS, ROWS, 2 * BEAMS), f32),
            pltpu.VMEM((1024, 128), f32),
            pltpu.VMEM((128, BEAMS), f32),
            pltpu.VMEM((32, 8, 128), bf16),
            pltpu.VMEM((32, 8, 128), bf16),
            pltpu.VMEM((256, 128), f32),
            pltpu.VMEM((16, 16, 128), bf16),
            pltpu.VMEM((16, 16, 128), bf16),
            pltpu.VMEM((16, 2048), bf16),
            pltpu.VMEM((144, 128), f32),
            pltpu.VMEM((144, 128), f32),
            pltpu.VMEM((TAPS * 128, 256), bf16),
            pltpu.VMEM((2048, 2048), bf16),
            pltpu.VMEM((2, 8, 24, 128), f32),
            pltpu.VMEM((2, 72 * 16, 128), bf16),
            pltpu.VMEM((256, 256), f32),
            pltpu.VMEM((16, 16, 128), bf16),
            pltpu.VMEM((16, 16, 128), bf16),
            dma((6,)),
            dma((16,)),
            dma((16,)),
            dma((32,)),
            dma((32,)),
            dma((16,)),
            dma((16,)),
            dma((16,)),
            dma((16,)),
            pltpu.SemaphoreType.REGULAR,
        ],
        compiler_params=pltpu.CompilerParams(
            collective_id=0, has_side_effects=True, vmem_limit_bytes=60 * 1024 * 1024
        ),
    )(jnp.asarray(start_powers()), rep_len, spectra, col_lags, row_lags, replica, factors)


def on_device(spectra, row_lags, col_lags, replica, rep_len):
    returned = ping(spectra, row_lags, col_lags, replica, rep_len)
    return jnp.transpose(returned.reshape(16, 8, 2, 128), (0, 2, 1, 3)).reshape(16, 2, BINS)


def solution(mesh):
    placed = (P(None, "tm", "freq", "hyd"), P(), P(), P(), P())
    return jax.shard_map(
        on_device,
        mesh=mesh,
        in_specs=placed,
        out_specs=P(("hyd", "freq"), None, "tm"),
        check_vma=False,
    )
```
